128 devices in a mesh: slab: 4 (over y_lo, core), tile: 32 (over z, y_hi, x).
Axes of the slice: x: 4, y: 4 (y_hi: 2, y_lo: 2; y = y_hi * 2 + y_lo), z: 4, core: 2. Of those that a mesh axis runs over, the one named last changes fastest.
Arguments:
- electric: float32 [3, 56, 1024, 1024], P(None, 'slab', 'tile'), may hold values from -6 to 6
- current: float32 [3, 56, 1024, 1024], P(None, 'slab', 'tile'), may hold values from -6 to 6
- mass_shift: float32 [56, 1024, 1024], P('slab', 'tile'), may hold values from 0.5 to 4
- interface: float32 [4, 2, 2, 1024, 1024], P('slab', None, None, 'tile'), may hold values from -6 to 6
- auxiliary: float32 [4, 2, 4, 2, 1024, 1024], P('slab', None, None, None, 'tile'), may hold values from -3 to 3
Outputs:
- smoothed: float32 [3, 56, 1024, 1024], P(None, 'slab', 'tile')
- next_interface: float32 [4, 2, 2, 1024, 1024], P('slab', None, None, 'tile')
- next_auxiliary: float32 [4, 2, 4, 2, 1024, 1024], P('slab', None, None, None, 'tile')
The draws below stay inside these ranges and needn't reach their ends.
All inputs are finite; a program needn't handle non-finite values.
Results may differ from the reference program's by a relative error of at most 0.0001.
Values sent between devices are 32-bit elements; how exact they have to be, the bound alone decides.
A program may use at most 128 MiB of HBM per device.

```python
import math
import jax
import jax.numpy as jnp
from jax import lax

X = 1024
PZ = 14
SLABS = 4
NY = 1024
NZ = 56


def shard_levels(rng, dims, pieces, smallest, largest):
    def one(dim, parts):
        draws = jax.random.uniform(jax.random.fold_in(jax.random.fold_in(rng, 6), dim), (parts,), jnp.float32, smallest / len(pieces), largest / len(pieces))
        return jnp.repeat(jnp.exp(draws), dims[dim] // parts).reshape((-1,) + (1,) * (len(dims) - dim - 1))

    level = one(*pieces[0])
    for cut in pieces[1:]:
        level = level * one(*cut)
    return level


def normal_values(rng, extent, spread, reach, shards=(), dtype=jnp.bfloat16):
    factor_of = shard_levels(rng, extent, shards, -0.22, 0.18) if shards else 1.0
    result = jax.random.normal(rng, extent, jnp.float32) * spread * factor_of
    return jnp.minimum(jnp.maximum(result, -reach), reach).astype(dtype)


def setup_inputs(seed: int = 0) -> dict:
    splits = jax.random.split(jax.random.key(seed), 6)
    return {
        "electric": normal_values(splits[0], (3, NZ, NY, X), 1.0, 6.0, ((1, 4), (2, 32)), jnp.float32),
        "current": normal_values(splits[1], (3, NZ, NY, X), 1.0, 6.0, ((1, 4), (2, 32)), jnp.float32),
        "mass_shift": jnp.clip(jnp.exp(math.log(4.0) - 2.0794415 * jax.random.uniform(splits[2], (NZ, NY, X), jnp.float32) ** shard_levels(splits[2], (NZ, NY, X), ((0, 4), (1, 32)), -0.2, 0.2)), 0.5, 4.0),
        "interface": normal_values(splits[3], (SLABS, 2, 2, NY, X), 1.0, 6.0, ((0, 4), (3, 32)), jnp.float32),
        "auxiliary": normal_values(splits[4], (SLABS, 2, 4, 2, NY, X), 0.5, 3.0, ((0, 4), (4, 32)), jnp.float32),
    }


pade_weights = [2.0 / 9.0 * math.sin(j * math.pi / 9.0) ** 2 for j in range(1, 5)]
pade_decays = [math.cos(j * math.pi / 9.0) ** 2 for j in range(1, 5)]


def forward_diff(values, along):
    along = along % values.ndim
    count = values.shape[along]
    shifted = jnp.concatenate([lax.slice_in_dim(values, 1, count, axis=along), jnp.zeros_like(lax.slice_in_dim(values, 0, 1, axis=along))], along)
    return shifted - values


def backward_diff(values, along):
    along = along % values.ndim
    count = values.shape[along]
    shifted = jnp.concatenate([jnp.zeros_like(lax.slice_in_dim(values, 0, 1, axis=along)), lax.slice_in_dim(values, 0, count - 1, axis=along)], along)
    return values - shifted


def curl_curl(padded):
    field_x, field_y, field_z = padded[0], padded[1], padded[2]
    flux_x = forward_diff(field_z, 1) - forward_diff(field_y, 0)
    flux_y = forward_diff(field_x, 0) - forward_diff(field_z, 2)
    flux_z = forward_diff(field_y, 2) - forward_diff(field_x, 1)
    image_x = backward_diff(flux_z, 1) - backward_diff(flux_y, 0)
    image_y = backward_diff(flux_x, 0) - backward_diff(flux_z, 2)
    image_z = backward_diff(flux_y, 2) - backward_diff(flux_x, 1)
    return jnp.stack([image_x, image_y, image_z])[:, 1:-1, 1:-1, :]


def update(padded, current, mass_shift):
    interior = padded[:, 1:-1, 1:-1, :]
    residual = current - (curl_curl(padded) + mass_shift * interior)
    return interior + 0.5 * residual / (mass_shift + 4.0)


def surface(padded):
    comp_x = padded[..., 0, :, :]
    comp_y = padded[..., 1, :, :]
    divergence = backward_diff(comp_x, -1) + backward_diff(comp_y, -2)
    rotation = forward_diff(comp_y, -1) - forward_diff(comp_x, -2)
    vort_x = backward_diff(rotation, -2) - forward_diff(divergence, -1)
    vort_y = -backward_diff(rotation, -1) - forward_diff(divergence, -2)
    return (jnp.stack([vort_x, vort_y], axis=-3) / 8.0)[..., 1:-1, :]


def reference(electric, current, mass_shift, interface, auxiliary):
    weights = jnp.asarray(pade_weights, jnp.float32).reshape(1, 4, 1, 1, 1)
    decays = jnp.asarray(pade_decays, jnp.float32).reshape(1, 4, 1, 1, 1)
    fields = []
    outgoing_all = []
    auxiliary_all = []
    for slab_index in range(SLABS):
        planes = slice(slab_index * PZ, (slab_index + 1) * PZ)
        local_field = electric[:, planes]
        local_current = current[:, planes]
        local_shift = mass_shift[planes]
        zero_plane = jnp.zeros((1, NY, X), jnp.float32)
        below_ghost = jnp.concatenate([interface[slab_index, 0], zero_plane], 0)
        above_ghost = jnp.concatenate([interface[slab_index, 1], zero_plane], 0)
        for sweep_index in range(2):
            extended = jnp.concatenate([below_ghost[:, None], local_field, above_ghost[:, None]], 1)
            padded = jnp.pad(extended, ((0, 0), (0, 0), (1, 1), (0, 0)))
            local_field = update(padded, local_current, local_shift)
        fields.append(local_field)
        traces = jnp.stack([local_field[0:2, 0], local_field[0:2, -1]])
        combined = traces[:, None] - decays * auxiliary[slab_index]
        padded_surface = jnp.pad(combined, ((0, 0), (0, 0), (0, 0), (1, 1), (0, 0)))
        new_auxiliary = surface(padded_surface)
        auxiliary_all.append(new_auxiliary)
        outgoing_all.append(traces + jnp.sum(weights * new_auxiliary, axis=1))
    zero_face = jnp.zeros((2, NY, X), jnp.float32)
    interfaces = []
    for slab_index in range(SLABS):
        from_below = outgoing_all[slab_index - 1][1] if slab_index > 0 else zero_face
        from_above = outgoing_all[slab_index + 1][0] if slab_index < SLABS - 1 else zero_face
        interfaces.append(jnp.stack([from_below, from_above]))
    return jnp.concatenate(fields, axis=1), jnp.stack(interfaces), jnp.stack(auxiliary_all)
```

```python
import functools
import math

import jax
import jax.numpy as jnp
from jax import lax
from jax.experimental import pallas as pl
from jax.experimental.pallas import tpu as pltpu
from jax.sharding import PartitionSpec as P

MESH = pl.DeviceIdType.MESH
TERMS = 4
pade_weights = [2.0 / 9.0 * math.sin(j * math.pi / 9.0) ** 2 for j in range(1, 5)]
pade_decays = [math.cos(j * math.pi / 9.0) ** 2 for j in range(1, 5)]
LANES = 128
PAD = 8


def kernel(
    n_slab,
    n_tile,
    electric,
    current,
    mass,
    interface,
    auxiliary,
    smoothed,
    next_if,
    next_aux,
    e0,
    e1,
    cur,
    mg,
    ax,
    tr,
    osum,
    out,
    pu1,
    pd1,
    ru1,
    rd1,
    pua,
    pda,
    rua,
    rda,
    pu2,
    pd2,
    ru2,
    rd2,
    pu3,
    pd3,
    ru3,
    rd3,
    load_sem,
    send_sem,
    recv_sem,
):
    planes, rows, width = electric.shape[1:]
    cols = width // LANES
    tiles = rows // 8
    depth = planes + 2
    tall = rows + 2 * PAD
    pitch = cols * tall
    last = PAD + rows - 1
    slab = lax.axis_index("slab")
    tile = lax.axis_index("tile")
    has_up = tile < n_tile - 1
    has_dn = tile > 0
    slab_up = slab < n_slab - 1
    slab_dn = slab > 0
    up = {"tile": tile + 1}
    dn = {"tile": tile - 1}
    sup = {"slab": slab + 1}
    sdn = {"slab": slab - 1}

    def columns(ref, c):
        return ref.at[..., pl.ds(c * LANES, LANES)]

    body = pl.ds(PAD, rows)
    e_loads = [
        pltpu.make_async_copy(
            columns(electric, c), e0.at[:, pl.ds(1, planes), c, body, :], load_sem.at[0, c]
        )
        for c in range(cols)
    ]
    ghosts = []
    for i, buf in enumerate((e0, e1)):
        for side in range(2):
            for c in range(cols):
                ghosts.append(
                    pltpu.make_async_copy(
                        columns(interface, c).at[0, side],
                        buf.at[pl.ds(0, 2), side * (depth - 1), c, body, :],
                        load_sem.at[1 + 2 * i + side, c],
                    )
                )
    a_loads = [
        pltpu.make_async_copy(
            columns(auxiliary, c).at[0], ax.at[:, :, :, c, body, :], load_sem.at[5, c]
        )
        for c in range(cols)
    ]
    m_load = pltpu.make_async_copy(mass, mg, load_sem.at[6, 0])
    c_load = pltpu.make_async_copy(current, cur, load_sem.at[6, 1])
    for copy in (*e_loads, *ghosts, *a_loads, m_load, c_load):
        copy.start()

    barrier = pltpu.get_barrier_semaphore()
    for there, who in ((has_up, up), (has_dn, dn), (slab_up, sup), (slab_dn, sdn)):

        @pl.when(there)
        def _():
            pl.semaphore_signal(barrier, inc=1, device_id=who, device_id_type=MESH)

    def exchange(slot, src_up, dst_up, src_dn, dst_dn):
        goes_up = pltpu.make_async_remote_copy(
            src_ref=src_up,
            dst_ref=dst_up,
            send_sem=send_sem.at[slot, 0],
            recv_sem=recv_sem.at[slot, 0],
            device_id=up,
            device_id_type=MESH,
        )
        goes_dn = pltpu.make_async_remote_copy(
            src_ref=src_dn,
            dst_ref=dst_dn,
            send_sem=send_sem.at[slot, 1],
            recv_sem=recv_sem.at[slot, 1],
            device_id=dn,
            device_id_type=MESH,
        )
        return goes_up, goes_dn

    def start(pair):
        @pl.when(has_up)
        def _():
            pair[0].start()

        @pl.when(has_dn)
        def _():
            pair[1].start()

    def arrived(pair):
        @pl.when(has_dn)
        def _():
            pair[0].wait_recv()

        @pl.when(has_up)
        def _():
            pair[1].wait_recv()

    def sent(pair):
        @pl.when(has_up)
        def _():
            pair[0].wait_send()

        @pl.when(has_dn)
        def _():
            pair[1].wait_send()

    first = exchange(0, pu1, ru1, pd1, rd1)
    aux_rows = exchange(1, pua, rua, pda, rda)
    second = exchange(2, pu2, ru2, pd2, rd2)
    third = exchange(3, pu3, ru3, pd3, rd3)
    slab_goes_up = pltpu.make_async_remote_copy(
        src_ref=out.at[1],
        dst_ref=next_if.at[0, 0],
        send_sem=send_sem.at[4, 0],
        recv_sem=recv_sem.at[4, 0],
        device_id=sup,
        device_id_type=MESH,
    )
    slab_goes_dn = pltpu.make_async_remote_copy(
        src_ref=out.at[0],
        dst_ref=next_if.at[0, 1],
        send_sem=send_sem.at[4, 1],
        recv_sem=recv_sem.at[4, 1],
        device_id=sdn,
        device_id_type=MESH,
    )

    flat0 = e0.reshape(3 * depth * pitch, LANES)
    flat1 = e1.reshape(3 * depth * pitch, LANES)
    flata = ax.reshape(2 * TERMS * 2 * pitch, LANES)
    flatt = tr.reshape(4 * pitch, LANES)
    zero_row = jnp.zeros((cols, LANES), jnp.float32)
    zero_tile = jnp.zeros((8, LANES), jnp.float32)

    def line(plane, row):
        return pl.ds(plane * pitch + row, cols, stride=tall)

    for buf in (e0, e1):
        for c in range(cols):
            for r in range(tall // 8):
                buf[2, 0, c, pl.ds(8 * r, 8), :] = zero_tile

    @pl.when(jnp.logical_not(has_dn))
    def _():
        for comp in range(3):

            @pl.loop(1, depth)
            def _(p):
                flat0[line(comp * depth + p, PAD - 1), :] = zero_row
                flat1[line(comp * depth + p, PAD - 1), :] = zero_row

        @pl.loop(0, 2 * TERMS * 2)
        def _(p):
            flata[line(p, PAD - 1), :] = zero_row

        for p in range(4):
            flatt[line(p, PAD - 1), :] = zero_row

    @pl.when(jnp.logical_not(has_up))
    def _():
        for comp in (0, 2):

            @pl.loop(1, depth)
            def _(p):
                flat0[line(comp * depth + p, last + 1), :] = zero_row
                flat1[line(comp * depth + p, last + 1), :] = zero_row

        @pl.loop(0, 2 * TERMS * 2)
        def _(p):
            flata[line(p, last + 1), :] = zero_row

        for p in range(4):
            flatt[line(p, last + 1), :] = zero_row

    @pl.when(jnp.logical_not(slab_dn))
    def _():
        next_if[0, 0] = jnp.zeros(next_if.shape[2:], jnp.float32)

    @pl.when(jnp.logical_not(slab_up))
    def _():
        next_if[0, 1] = jnp.zeros(next_if.shape[2:], jnp.float32)

    def pack(flat, to_up, to_dn):
        @pl.loop(0, planes)
        def _(k):
            for comp in range(3):
                to_up[comp * planes + k] = flat[line(comp * depth + 1 + k, last), :]
            for i, comp in enumerate((0, 2)):
                to_dn[i * planes + k] = flat[line(comp * depth + 1 + k, PAD), :]

    def unpack(flat, from_dn, from_up):
        @pl.when(has_dn)
        def _():
            @pl.loop(0, planes)
            def _(k):
                for comp in range(3):
                    flat[line(comp * depth + 1 + k, PAD - 1), :] = from_dn[comp * planes + k]

        @pl.when(has_up)
        def _():
            @pl.loop(0, planes)
            def _(k):
                for i, comp in enumerate((0, 2)):
                    flat[line(comp * depth + 1 + k, last + 1), :] = from_up[i * planes + k]

    lane = lax.broadcasted_iota(jnp.int32, (8, LANES), 1)
    not_last = lane < LANES - 1
    not_first = lane > 0

    def ahead(values):
        turned = [pltpu.roll(v, LANES - 1, 1) for v in values] + [zero_tile]
        return [jnp.where(not_last, turned[c], turned[c + 1]) for c in range(cols)]

    def behind(values):
        turned = [zero_tile] + [pltpu.roll(v, 1, 1) for v in values]
        return [jnp.where(not_first, turned[c + 1], turned[c]) for c in range(cols)]

    def sweep(src, k, r, first_sweep):
        top = PAD + 8 * r

        def take(comp, step_z, step_y):
            p = k + 1 + step_z
            return [src[comp, p, c, pl.ds(top + step_y, 8), :] for c in range(cols)]

        ex, ey, ez = take(0, 0, 0), take(1, 0, 0), take(2, 0, 0)
        exjp = take(0, 0, 1)
        eyr = ahead(ey)
        hz = [eyr[c] - ey[c] - exjp[c] + ex[c] for c in range(cols)]
        hzl = behind(hz)
        ezjp, eykp = take(2, 0, 1), take(1, 1, 0)
        ezkm, ezjpkm, eykm = take(2, -1, 0), take(2, -1, 1), take(1, -1, 0)
        hx = [(ezjp[c] - ez[c]) - (eykp[c] - ey[c]) for c in range(cols)]
        hxkm = [(ezjpkm[c] - ezkm[c]) - (ey[c] - eykm[c]) for c in range(cols)]
        image_y = [(hx[c] - hxkm[c]) - (hz[c] - hzl[c]) for c in range(cols)]
        eyjm = take(1, 0, -1)
        t = [(ey[c] - eyjm[c]) + (ez[c] - ezkm[c]) for c in range(cols)]
        tn = ahead(t)
        exjm, exkp, exkm = take(0, 0, -1), take(0, 1, 0), take(0, -1, 0)
        image_x = [
            (tn[c] - t[c]) + (4.0 * ex[c] - ((exjp[c] + exjm[c]) + (exkp[c] + exkm[c])))
            for c in range(cols)
        ]
        ezr = ahead(ez)
        hy = [(exkp[c] - ex[c]) - (ezr[c] - ez[c]) for c in range(cols)]
        hyl = behind(hy)
        ezjm, eyjmkp = take(2, 0, -1), take(1, 1, -1)
        hxjm = [(ez[c] - ezjm[c]) - (eyjmkp[c] - eyjm[c]) for c in range(cols)]
        image_z = [(hy[c] - hyl[c]) - (hx[c] - hxjm[c]) for c in range(cols)]
        news = []
        for c in range(cols):
            place = (k, pl.ds(8 * r, 8), pl.ds(c * LANES, LANES))
            if first_sweep:
                g = 0.5 / (mg[place] + 4.0)
                mg[place] = g
            else:
                g = mg[place]
            keep = 0.5 + 4.0 * g
            news.append(
                [
                    keep * old[c] + g * (cur[(comp, *place)] - image[c])
                    for comp, (old, image) in enumerate(
                        ((ex, image_x), (ey, image_y), (ez, image_z))
                    )
                ]
            )
        return news

    def first_sweep(which):
        @pl.loop(0, planes)
        def _(k):
            for r in which:
                news = sweep(e0, k, r, True)
                for c in range(cols):
                    for comp in range(3):
                        e1[comp, k + 1, c, pl.ds(PAD + 8 * r, 8), :] = news[c][comp]

    def second_sweep_inner(which):
        @pl.loop(1, planes - 1)
        def _(k):
            for r in which:
                news = sweep(e1, k, r, False)
                for c in range(cols):
                    for comp in range(3):
                        smoothed[
                            comp, k, pl.ds(8 * r, 8), pl.ds(c * LANES, LANES)
                        ] = news[c][comp]

    def second_sweep_ends(which):
        @pl.loop(0, 2)
        def _(side):
            k = side * (planes - 1)
            for r in which:
                news = sweep(e1, k, r, False)
                for c in range(cols):
                    for comp in range(3):
                        smoothed[
                            comp, k, pl.ds(8 * r, 8), pl.ds(c * LANES, LANES)
                        ] = news[c][comp]
                    for comp in range(2):
                        tr[side * 2 + comp, c, pl.ds(PAD + 8 * r, 8), :] = news[c][comp]

    edge_last = jnp.where(lane == LANES - 1, 3.0, 4.0)
    edge_first = jnp.where(lane == 0, 3.0, 4.0)

    def surface(read, comp, r):
        top = PAD + 8 * r
        u = [read(c, top) for c in range(cols)]
        ua, ub = ahead(u), behind(u)
        result = []
        for c in range(cols):
            if comp == 0 and c == cols - 1:
                centre = edge_last * u[c]
            elif comp == 1 and c == 0:
                centre = edge_first * u[c]
            else:
                centre = 4.0 * u[c]
            around = (ua[c] + ub[c]) + (read(c, top + 1) + read(c, top - 1))
            result.append(0.125 * (centre - around))
        return u, result

    def aux_surface(which):
        @pl.loop(0, 2)
        def _(side):
            for comp in range(2):
                for r in which:
                    total = [zero_tile] * cols
                    for j in range(TERMS):

                        def read(c, row):
                            return ax[side, j, comp, c, pl.ds(row, 8), :]

                        _, image = surface(read, comp, r)
                        for c in range(cols):
                            part = pade_decays[j] * image[c]
                            place = (pl.ds(8 * r, 8), pl.ds(c * LANES, LANES))
                            next_aux[(0, side, j, comp, *place)] = part
                            total[c] = total[c] + pade_weights[j] * part
                    for c in range(cols):
                        place = (pl.ds(8 * r, 8), pl.ds(c * LANES, LANES))
                        osum[(side, comp, *place)] = total[c]

    peers = sum(jnp.where(there, 1, 0) for there in (has_up, has_dn, slab_up, slab_dn))
    pl.semaphore_wait(barrier, peers)

    for copy in (*e_loads, *ghosts):
        copy.wait()
    pack(flat0, pu1, pd1)
    pu1[3 * planes] = flat0[line(depth + planes + 1, last), :]
    start(first)

    for copy in a_loads:
        copy.wait()

    @pl.loop(0, 2 * TERMS * 2)
    def _(p):
        pua[p] = flata[line(p, last), :]
        pda[p] = flata[line(p, PAD), :]

    start(aux_rows)
    m_load.wait()
    c_load.wait()
    inner = tuple(range(1, tiles - 1))
    outer = (0, tiles - 1)
    first_sweep(inner)
    arrived(first)
    unpack(flat0, ru1, rd1)

    @pl.when(has_dn)
    def _():
        row = ru1[3 * planes]
        flat0[line(depth + planes + 1, PAD - 1), :] = row
        flat1[line(depth + planes + 1, PAD - 1), :] = row

    first_sweep(outer)
    pack(flat1, pu2, pd2)
    start(second)

    aux_surface(inner)
    arrived(aux_rows)

    @pl.when(has_dn)
    def _():
        @pl.loop(0, 2 * TERMS * 2)
        def _(p):
            flata[line(p, PAD - 1), :] = rua[p]

    @pl.when(has_up)
    def _():
        @pl.loop(0, 2 * TERMS * 2)
        def _(p):
            flata[line(p, last + 1), :] = rda[p]

    aux_surface(outer)
    second_sweep_ends(inner)
    second_sweep_inner(inner)
    arrived(second)
    unpack(flat1, ru2, rd2)
    second_sweep_ends(outer)
    for p in range(4):
        pu3[p] = flatt[line(p, last), :]
        pd3[p] = flatt[line(p, PAD), :]
    start(third)
    second_sweep_inner(outer)
    arrived(third)

    @pl.when(has_dn)
    def _():
        for p in range(4):
            flatt[line(p, PAD - 1), :] = ru3[p]

    @pl.when(has_up)
    def _():
        for p in range(4):
            flatt[line(p, last + 1), :] = rd3[p]

    weight = sum(pade_weights)

    @pl.loop(0, 2)
    def _(side):
        for comp in range(2):
            for r in range(tiles):

                def read(c, row):
                    return tr[side * 2 + comp, c, pl.ds(row, 8), :]

                u, image = surface(read, comp, r)
                for c in range(cols):
                    place = (pl.ds(8 * r, 8), pl.ds(c * LANES, LANES))
                    out[(side, comp, *place)] = (
                        u[c] + weight * image[c] - osum[(side, comp, *place)]
                    )
                    osum[(side, comp, *place)] = image[c]

    @pl.when(slab_up)
    def _():
        slab_goes_up.start()

    @pl.when(slab_dn)
    def _():
        slab_goes_dn.start()

    @pl.loop(0, 2)
    def _(side):
        for comp in range(2):
            for r in range(tiles):
                for c in range(cols):
                    place = (pl.ds(8 * r, 8), pl.ds(c * LANES, LANES))
                    image = osum[(side, comp, *place)]
                    for j in range(TERMS):
                        where = (0, side, j, comp, *place)
                        next_aux[where] = image - next_aux[where]

    for pair in (first, aux_rows, second, third):
        sent(pair)

    @pl.when(slab_dn)
    def _():
        slab_goes_up.wait_recv()
        slab_goes_dn.wait_send()

    @pl.when(slab_up)
    def _():
        slab_goes_dn.wait_recv()
        slab_goes_up.wait_send()


def solution(mesh):
    n_slab, n_tile = mesh.shape["slab"], mesh.shape["tile"]

    def step(electric, current, mass_shift, interface, auxiliary):
        _, planes, rows, width = electric.shape
        cols = width // LANES
        tall = rows + 2 * PAD
        f32 = jnp.float32
        hbm = pl.BlockSpec(memory_space=pltpu.MemorySpace.HBM)
        vmem = pl.BlockSpec(memory_space=pltpu.VMEM)

        def lines(n):
            return pltpu.VMEM((n, cols, LANES), f32)

        return pl.pallas_call(
            functools.partial(kernel, n_slab, n_tile),
            out_shape=(
                pltpu.VMEM(electric.shape, f32),
                pltpu.VMEM(interface.shape, f32),
                pltpu.VMEM(auxiliary.shape, f32),
            ),
            in_specs=[hbm] * 5,
            out_specs=(vmem, vmem, vmem),
            scratch_shapes=[
                pltpu.VMEM((3, planes + 2, cols, tall, LANES), f32),
                pltpu.VMEM((3, planes + 2, cols, tall, LANES), f32),
                pltpu.VMEM(electric.shape, f32),
                pltpu.VMEM(mass_shift.shape, f32),
                pltpu.VMEM((2, TERMS, 2, cols, tall, LANES), f32),
                pltpu.VMEM((4, cols, tall, LANES), f32),
                pltpu.VMEM((2, 2, rows, width), f32),
                pltpu.VMEM((2, 2, rows, width), f32),
                lines(3 * planes + 1),
                lines(2 * planes),
                lines(3 * planes + 1),
                lines(2 * planes),
                lines(4 * TERMS),
                lines(4 * TERMS),
                lines(4 * TERMS),
                lines(4 * TERMS),
                lines(3 * planes),
                lines(2 * planes),
                lines(3 * planes),
                lines(2 * planes),
                lines(4),
                lines(4),
                lines(4),
                lines(4),
                pltpu.SemaphoreType.DMA((7, cols)),
                pltpu.SemaphoreType.DMA((5, 2)),
                pltpu.SemaphoreType.DMA((5, 2)),
            ],
            compiler_params=pltpu.CompilerParams(
                collective_id=0, has_side_effects=True, vmem_limit_bytes=44 * 2**20
            ),
        )(electric, current, mass_shift, interface, auxiliary)

    placed = (
        P(None, "slab", "tile", None),
        P(None, "slab", "tile", None),
        P("slab", "tile", None),
        P("slab", None, None, "tile", None),
        P("slab", None, None, None, "tile", None),
    )
    return jax.shard_map(
        step,
        mesh=mesh,
        in_specs=placed,
        out_specs=(
            P(None, "slab", "tile", None),
            P("slab", None, None, "tile", None),
            P("slab", None, None, None, "tile", None),
        ),
        check_vma=False,
    )
```

```python
import functools
import math

import jax
import jax.numpy as jnp
from jax import lax
from jax.experimental import pallas as pl
from jax.experimental.pallas import tpu as pltpu
from jax.sharding import PartitionSpec as P

MESH = pl.DeviceIdType.MESH
TERMS = 4
pade_weights = [2.0 / 9.0 * math.sin(j * math.pi / 9.0) ** 2 for j in range(1, 5)]
pade_decays = [math.cos(j * math.pi / 9.0) ** 2 for j in range(1, 5)]
LANES = 128
PAD = 8
VMEM_LIMIT = 55 * 2**20 + 2**19


PAIRS = 2


def kernel(
    n_slab,
    n_tile,
    electric,
    current,
    mass,
    interface,
    auxiliary,
    smoothed,
    next_if,
    next_aux,
    e0,
    e1,
    cur,
    mg,
    ax,
    tr,
    osum,
    out,
    pu1,
    pd1,
    ru1,
    rd1,
    pua,
    pda,
    rua,
    rda,
    pu2,
    pd2,
    ru2,
    rd2,
    load_sem,
    send_sem,
    recv_sem,
):
    planes, rows, width = electric.shape[1:]
    cols = width // LANES
    tiles = rows // 8
    depth = planes + 2
    tall = rows + 2 * PAD
    pitch = cols * tall
    last = PAD + rows - 1
    inner = tuple(range(1, tiles - 1))
    outer = (0, tiles - 1)
    slab = lax.axis_index("slab")
    tile = lax.axis_index("tile")
    has_up = tile < n_tile - 1
    has_dn = tile > 0
    slab_up = slab < n_slab - 1
    slab_dn = slab > 0
    up = {"tile": tile + 1}
    dn = {"tile": tile - 1}
    sup = {"slab": slab + 1}
    sdn = {"slab": slab - 1}

    def columns(ref, c):
        return ref.at[..., pl.ds(c * LANES, LANES)]

    body = pl.ds(PAD, rows)

    def field_load(c, slot, row, count):
        return pltpu.make_async_copy(
            electric.at[:, :, pl.ds(row, count), pl.ds(c * LANES, LANES)],
            e0.at[:, pl.ds(1, planes), c, pl.ds(PAD + row, count), :],
            load_sem.at[slot, c],
        )

    edge_loads = [field_load(c, 0, 0, 8) for c in range(cols)]
    edge_loads += [field_load(c, 1, rows - 8, 8) for c in range(cols)]
    inner_loads = [field_load(c, 2, 8, rows - 16) for c in range(cols)]

    def ghost_loads(buf, slot):
        return [
            pltpu.make_async_copy(
                columns(interface, c).at[0, side],
                buf.at[pl.ds(0, 2), side * (depth - 1), c, body, :],
                load_sem.at[slot + side, c],
            )
            for side in range(2)
            for c in range(cols)
        ]

    ghosts0, ghosts1 = ghost_loads(e0, 3), ghost_loads(e1, 5)
    aux_loads = [
        pltpu.make_async_copy(
            columns(auxiliary, c).at[0], ax.at[:, :, :, c, body, :], load_sem.at[7, c]
        )
        for c in range(cols)
    ]
    m_load = pltpu.make_async_copy(mass, mg, load_sem.at[8, 0])
    c_load = pltpu.make_async_copy(current, cur, load_sem.at[8, 1])
    for copy in (*edge_loads, *ghosts0):
        copy.start()

    barrier = pltpu.get_barrier_semaphore()
    for there, who in ((has_up, up), (has_dn, dn), (slab_up, sup), (slab_dn, sdn)):

        @pl.when(there)
        def _():
            pl.semaphore_signal(barrier, inc=1, device_id=who, device_id_type=MESH)

    for copy in (*inner_loads, m_load, c_load, *ghosts1, *aux_loads):
        copy.start()

    def exchange(slot, src_up, dst_up, src_dn, dst_dn):
        goes_up = pltpu.make_async_remote_copy(
            src_ref=src_up,
            dst_ref=dst_up,
            send_sem=send_sem.at[slot, 0],
            recv_sem=recv_sem.at[slot, 0],
            device_id=up,
            device_id_type=MESH,
        )
        goes_dn = pltpu.make_async_remote_copy(
            src_ref=src_dn,
            dst_ref=dst_dn,
            send_sem=send_sem.at[slot, 1],
            recv_sem=recv_sem.at[slot, 1],
            device_id=dn,
            device_id_type=MESH,
        )
        return goes_up, goes_dn

    def part(slot, bufs, at, count):
        return exchange(slot, *(buf.at[pl.ds(at, count)] for buf in bufs))

    def start(pair):
        @pl.when(has_up)
        def _():
            pair[0].start()

        @pl.when(has_dn)
        def _():
            pair[1].start()

    def arrived(pair):
        @pl.when(has_dn)
        def _():
            pair[0].wait_recv()

        @pl.when(has_up)
        def _():
            pair[1].wait_recv()

    def sent(pair):
        @pl.when(has_up)
        def _():
            pair[0].wait_send()

        @pl.when(has_dn)
        def _():
            pair[1].wait_send()

    far = planes - 3
    near1 = ((0, 2, 0), (far, planes, 4))
    rest1 = ((2, far, 10),)
    near2 = ((0, 1, 0), (planes - 2, planes, 2))
    rest2 = ((1, planes - 2, 12),)
    first_near = part(0, (pu1, ru1, pd1, rd1), 0, 10)
    first_rest = part(1, (pu1, ru1, pd1, rd1), 10, 2 * (planes - 5))
    aux_rows = exchange(2, pua, rua, pda, rda)
    second_near = part(3, (pu2, ru2, pd2, rd2), 0, 12)
    second_rest = part(4, (pu2, ru2, pd2, rd2), 12, 2 * (planes - 3))
    slab_goes_up = pltpu.make_async_remote_copy(
        src_ref=out.at[1],
        dst_ref=next_if.at[0, 0],
        send_sem=send_sem.at[5, 0],
        recv_sem=recv_sem.at[5, 0],
        device_id=sup,
        device_id_type=MESH,
    )
    slab_goes_dn = pltpu.make_async_remote_copy(
        src_ref=out.at[0],
        dst_ref=next_if.at[0, 1],
        send_sem=send_sem.at[5, 1],
        recv_sem=recv_sem.at[5, 1],
        device_id=sdn,
        device_id_type=MESH,
    )

    flat0 = e0.reshape(3 * depth * pitch, LANES)
    flat1 = e1.reshape(3 * depth * pitch, LANES)
    flata = ax.reshape(2 * TERMS * 2 * pitch, LANES)
    flatt = tr.reshape(6 * pitch, LANES)
    zero_row = jnp.zeros((cols, LANES), jnp.float32)
    zero_tile = jnp.zeros((8, LANES), jnp.float32)

    def line(plane, row):
        return pl.ds(plane * pitch + row, cols, stride=tall)

    for buf in (e0, e1):
        for c in range(cols):
            for r in range(tall // 8):
                buf[2, 0, c, pl.ds(8 * r, 8), :] = zero_tile

    @pl.loop(1, depth)
    def _(p):
        for flat in (flat0, flat1):
            for comp in range(3):
                flat[line(comp * depth + p, PAD - 1), :] = zero_row
            for comp in (0, 2):
                flat[line(comp * depth + p, last + 1), :] = zero_row

    @pl.loop(0, 2 * TERMS * 2)
    def _(p):
        flata[line(p, PAD - 1), :] = zero_row
        flata[line(p, last + 1), :] = zero_row

    for p in range(4):
        flatt[line(p, PAD - 1), :] = zero_row
        flatt[line(p, last + 1), :] = zero_row

    @pl.when(jnp.logical_not(slab_dn))
    def _():
        next_if[0, 0] = jnp.zeros(next_if.shape[2:], jnp.float32)

    @pl.when(jnp.logical_not(slab_up))
    def _():
        next_if[0, 1] = jnp.zeros(next_if.shape[2:], jnp.float32)

    lane = lax.broadcasted_iota(jnp.int32, (8, LANES), 1)
    not_last = lane < LANES - 1
    not_first = lane > 0
    sub = lax.broadcasted_iota(jnp.int32, (cols, LANES), 0)
    row_lane = lax.broadcasted_iota(jnp.int32, (cols, LANES), 1)

    def row_ahead(row):
        turned = pltpu.roll(row, LANES - 1, 1)
        wrapped = jnp.where(sub < cols - 1, pltpu.roll(turned, cols - 1, 0), 0.0)
        return jnp.where(row_lane < LANES - 1, turned, wrapped)

    def row_behind(row):
        turned = pltpu.roll(row, 1, 1)
        wrapped = jnp.where(sub > 0, pltpu.roll(turned, 1, 0), 0.0)
        return jnp.where(row_lane > 0, turned, wrapped)

    def pack(flat, to_up, to_dn, spans):
        for low, high, at in spans:

            @pl.loop(low, high)
            def _(k):
                spot = at + PAIRS * (k - low)
                ey = flat[line(depth + 1 + k, last), :]
                over = flat[line(depth + 2 + k, last), :]
                to_up[spot] = (row_ahead(ey) - ey) + flat[line(1 + k, last), :]
                to_up[spot + 1] = flat[line(2 * depth + 1 + k, last), :] + (over - ey)
                to_dn[spot] = flat[line(1 + k, PAD), :]
                to_dn[spot + 1] = flat[line(2 * depth + 1 + k, PAD), :]

    def unpack(flat, from_dn, from_up, spans):
        for there, source, row in ((has_dn, from_dn, PAD - 1), (has_up, from_up, last + 1)):

            @pl.when(there)
            def _():
                for low, high, at in spans:

                    @pl.loop(low, high)
                    def _(k):
                        spot = at + PAIRS * (k - low)
                        flat[line(1 + k, row), :] = source[spot]
                        flat[line(2 * depth + 1 + k, row), :] = source[spot + 1]

    def back(value):
        return pltpu.roll(value, LANES - 1, 1)

    def forth(value):
        return pltpu.roll(value, 1, 1)

    def sweep(src, k, r, initial, write):
        top = PAD + 8 * r

        def at(comp, step_z, step_y, c):
            return src[comp, k + 1 + step_z, c, pl.ds(top + step_y, 8), :]

        def opening(c):
            if c == cols:
                return (None, None, None), (zero_tile,) * 3
            ey, ez = at(1, 0, 0, c), at(2, 0, 0, c)
            t = (ey - at(1, 0, -1, c)) + (ez - at(2, -1, 0, c))
            return (ey, ez, t), (back(ey), back(ez), back(t))

        here, turned = opening(0)
        hz_before = hy_before = zero_tile
        for c in range(cols):
            there, turned_there = opening(c + 1)
            ey, ez, t = here
            eyr, ezr, tn = (jnp.where(not_last, a, b) for a, b in zip(turned, turned_there))
            ex, exjp, exkp = at(0, 0, 0, c), at(0, 0, 1, c), at(0, 1, 0, c)
            hz = (eyr - ey) - (exjp - ex)
            hy = (exkp - ex) - (ezr - ez)
            hz_turned, hy_turned = forth(hz), forth(hy)
            dhz = hz - jnp.where(not_first, hz_turned, hz_before)
            dhy = hy - jnp.where(not_first, hy_turned, hy_before)
            place = (k, pl.ds(8 * r, 8), pl.ds(c * LANES, LANES))
            if initial:
                g = 0.5 / (mg[place] + 4.0)
                mg[place] = g
            else:
                g = mg[place]
            keep = 0.5 + 2.0 * g
            around = (exjp + at(0, 0, -1, c)) + (exkp + at(0, -1, 0, c))
            new_x = 0.5 * ex + g * ((cur[(0, *place)] + around) - (tn - t))
            eykp, ezjp = at(1, 1, 0, c), at(2, 0, 1, c)
            around = ((eykp + at(1, -1, 0, c)) - (ezjp - ez)) + (
                at(2, -1, 1, c) - at(2, -1, 0, c)
            )
            new_y = keep * ey + g * ((cur[(1, *place)] + around) + dhz)
            around = ((ezjp + at(2, 0, -1, c)) - (eykp - ey)) + (
                at(1, 1, -1, c) - at(1, 0, -1, c)
            )
            new_z = keep * ez + g * ((cur[(2, *place)] + around) - dhy)
            write(c, (new_x, new_y, new_z), g)
            here, turned = there, turned_there
            hz_before, hy_before = hz_turned, hy_turned

    def first_sweep(which, low, high, gap=0):
        @pl.loop(low, high)
        def _(step):
            k = step + (step // 2) * gap if gap else step
            for r in which:

                def write(c, news, g):
                    for comp in range(3):
                        e1[comp, k + 1, c, pl.ds(PAD + 8 * r, 8), :] = news[comp]

                sweep(e0, k, r, True, write)

    def second_sweep_inner(which):
        @pl.loop(1, planes - 1)
        def _(k):
            for r in which:

                def write(c, news, g):
                    place = (k, pl.ds(8 * r, 8), pl.ds(c * LANES, LANES))
                    for comp in range(3):
                        smoothed[(comp, *place)] = news[comp]

                sweep(e1, k, r, False, write)

    def second_sweep_ends(which):
        @pl.loop(0, 2)
        def _(side):
            k = side * (planes - 1)
            for r in which:

                def write(c, news, g):
                    place = (k, pl.ds(8 * r, 8), pl.ds(c * LANES, LANES))
                    for comp in range(3):
                        smoothed[(comp, *place)] = news[comp]
                    for comp in range(2):
                        tr[side * 2 + comp, c, pl.ds(PAD + 8 * r, 8), :] = news[comp]
                    tr[4 + side, c, pl.ds(PAD + 8 * r, 8), :] = g

                sweep(e1, k, r, False, write)

    edge_last = jnp.where(lane == LANES - 1, 3.0, 4.0)
    edge_first = jnp.where(lane == 0, 3.0, 4.0)

    def surface(read, comp, r, scale, write):
        top = PAD + 8 * r
        u = read(0, top)
        turned, before = back(u), zero_tile
        for c in range(cols):
            if c + 1 < cols:
                u_there = read(c + 1, top)
                turned_there = back(u_there)
            else:
                u_there, turned_there = None, zero_tile
            after = jnp.where(not_last, turned, turned_there)
            fore = forth(u)
            behind = jnp.where(not_first, fore, before)
            if comp == 0 and c == cols - 1:
                centre = (edge_last * (scale / 8)) * u
            elif comp == 1 and c == 0:
                centre = (edge_first * (scale / 8)) * u
            else:
                centre = (scale / 2) * u
            around = (after + behind) + (read(c, top + 1) + read(c, top - 1))
            write(c, u, centre - (scale / 8) * around)
            u, turned, before = u_there, turned_there, fore

    def aux_surface(which):
        @pl.loop(0, 2)
        def _(side):
            for comp in range(2):
                for r in which:
                    for j in range(TERMS):

                        def read(c, row):
                            return ax[side, j, comp, c, pl.ds(row, 8), :]

                        def write(c, u, image):
                            place = (pl.ds(8 * r, 8), pl.ds(c * LANES, LANES))
                            next_aux[(0, side, j, comp, *place)] = image
                            total = pade_weights[j] * image
                            if j:
                                total = osum[(side, comp, *place)] + total
                            osum[(side, comp, *place)] = total

                        surface(read, comp, r, pade_decays[j], write)

    peers = sum(jnp.where(there, 1, 0) for there in (has_up, has_dn, slab_up, slab_dn))
    pl.semaphore_wait(barrier, peers)

    for copy in (*edge_loads, *ghosts0):
        copy.wait()
    pack(flat0, pu1, pd1, near1)
    start(first_near)
    pack(flat0, pu1, pd1, rest1)
    start(first_rest)

    for copy in (*inner_loads, m_load, c_load):
        copy.wait()
    first_sweep(inner, 0, planes)
    for copy in (*ghosts1, *aux_loads):
        copy.wait()

    @pl.loop(0, 2 * TERMS * 2)
    def _(p):
        pua[p] = flata[line(p, last), :]
        pda[p] = flata[line(p, PAD), :]

    start(aux_rows)
    arrived(first_near)
    unpack(flat0, ru1, rd1, near1)
    first_sweep(outer, 0, 4, planes - 4)

    second_sweep_ends(outer)
    pack(flat1, pu2, pd2, near2)
    for p in range(6):
        pu2[6 + p] = flatt[line(p, last), :]
        pd2[6 + p] = flatt[line(p, PAD), :]
    start(second_near)

    arrived(first_rest)
    unpack(flat0, ru1, rd1, rest1)
    first_sweep(outer, 2, planes - 2)
    pack(flat1, pu2, pd2, rest2)
    start(second_rest)

    second_sweep_ends(inner)
    aux_surface(inner)
    arrived(aux_rows)
    for there, source, row in ((has_dn, rua, PAD - 1), (has_up, rda, last + 1)):

        @pl.when(there)
        def _():
            @pl.loop(0, 2 * TERMS * 2)
            def _(p):
                flata[line(p, row), :] = source[p]

    aux_surface(outer)

    arrived(second_near)
    unpack(flat1, ru2, rd2, near2)

    @pl.when(has_dn)
    def _():
        for side, (x, z, z_below) in enumerate(((0, 1, None), (4, 5, 3))):
            g = ru2[10 + side]
            row = pd2[x]
            slope = row - row_behind(row) + pd2[z]
            if z_below is not None:
                slope = slope - pd2[z_below]
            flatt[line(2 * side, PAD - 1), :] = ru2[6 + 2 * side] + g * row
            flatt[line(2 * side + 1, PAD - 1), :] = ru2[7 + 2 * side] - g * slope

    @pl.when(has_up)
    def _():
        for side, x in enumerate((0, 4)):
            g = rd2[10 + side]
            flatt[line(2 * side, last + 1), :] = rd2[6 + 2 * side] + g * pu2[x]
            flatt[line(2 * side + 1, last + 1), :] = rd2[7 + 2 * side]

    second_sweep_ends(outer)
    weight = sum(pade_weights)

    @pl.loop(0, 2)
    def _(side):
        for comp in range(2):
            for r in range(tiles):

                def read(c, row):
                    return tr[side * 2 + comp, c, pl.ds(row, 8), :]

                def write(c, u, image):
                    place = (side, comp, pl.ds(8 * r, 8), pl.ds(c * LANES, LANES))
                    out[place] = (u + weight * image) - osum[place]
                    osum[place] = image

                surface(read, comp, r, 1.0, write)

    @pl.when(slab_up)
    def _():
        slab_goes_up.start()

    @pl.when(slab_dn)
    def _():
        slab_goes_dn.start()

    second_sweep_inner(inner)

    @pl.loop(0, 2)
    def _(side):
        for comp in range(2):
            for r in range(tiles):
                for c in range(cols):
                    place = (pl.ds(8 * r, 8), pl.ds(c * LANES, LANES))
                    image = osum[(side, comp, *place)]
                    for j in range(TERMS):
                        where = (0, side, j, comp, *place)
                        next_aux[where] = image - next_aux[where]

    arrived(second_rest)
    unpack(flat1, ru2, rd2, rest2)
    second_sweep_inner(outer)

    for pair in (first_near, first_rest, aux_rows, second_near, second_rest):
        sent(pair)

    @pl.when(slab_dn)
    def _():
        slab_goes_up.wait_recv()
        slab_goes_dn.wait_send()

    @pl.when(slab_up)
    def _():
        slab_goes_dn.wait_recv()
        slab_goes_up.wait_send()


def store_kernel(field, face, aux, field_out, face_out, aux_out, sem):
    copies = [
        pltpu.make_async_copy(field.at[comp, pl.ds(k, half)], field_out.at[comp, pl.ds(k, half)], sem.at[i])
        for half in (field.shape[1] // 2,)
        for i, (comp, k) in enumerate((comp, k) for comp in range(3) for k in (0, half))
    ]
    copies += [
        pltpu.make_async_copy(aux.at[0, side, pl.ds(j, 2)], aux_out.at[0, side, pl.ds(j, 2)], sem.at[6 + 2 * side + j // 2])
        for side in range(2)
        for j in (0, 2)
    ]
    copies.append(pltpu.make_async_copy(face, face_out, sem.at[10]))
    for copy in copies:
        copy.start()
    for copy in copies:
        copy.wait()


def solution(mesh):
    n_slab, n_tile = mesh.shape["slab"], mesh.shape["tile"]

    def step(electric, current, mass_shift, interface, auxiliary):
        _, planes, rows, width = electric.shape
        cols = width // LANES
        tall = rows + 2 * PAD
        f32 = jnp.float32
        hbm = pl.BlockSpec(memory_space=pltpu.MemorySpace.HBM)
        vmem = pl.BlockSpec(memory_space=pltpu.VMEM)
        shapes = (electric.shape, interface.shape, auxiliary.shape)

        def lines(n):
            return pltpu.VMEM((n, cols, LANES), f32)

        held = pl.pallas_call(
            functools.partial(kernel, n_slab, n_tile),
            out_shape=tuple(pltpu.VMEM(shape, f32) for shape in shapes),
            in_specs=[hbm] * 5,
            out_specs=(vmem, vmem, vmem),
            scratch_shapes=[
                pltpu.VMEM((3, planes + 2, cols, tall, LANES), f32),
                pltpu.VMEM((3, planes + 2, cols, tall, LANES), f32),
                pltpu.VMEM(electric.shape, f32),
                pltpu.VMEM(mass_shift.shape, f32),
                pltpu.VMEM((2, TERMS, 2, cols, tall, LANES), f32),
                pltpu.VMEM((6, cols, tall, LANES), f32),
                pltpu.VMEM((2, 2, rows, width), f32),
                pltpu.VMEM((2, 2, rows, width), f32),
                *[lines(2 * planes)] * 4,
                *[lines(4 * TERMS)] * 4,
                *[lines(2 * planes + 6)] * 4,
                pltpu.SemaphoreType.DMA((9, cols)),
                pltpu.SemaphoreType.DMA((6, 2)),
                pltpu.SemaphoreType.DMA((6, 2)),
            ],
            compiler_params=pltpu.CompilerParams(
                collective_id=0, has_side_effects=True, vmem_limit_bytes=VMEM_LIMIT
            ),
        )(electric, current, mass_shift, interface, auxiliary)
        return pl.pallas_call(
            store_kernel,
            out_shape=tuple(jax.ShapeDtypeStruct(shape, f32) for shape in shapes),
            in_specs=[vmem] * 3,
            out_specs=(hbm, hbm, hbm),
            scratch_shapes=[pltpu.SemaphoreType.DMA((11,))],
            compiler_params=pltpu.CompilerParams(vmem_limit_bytes=2**20),
        )(*held)

    placed = (
        P(None, "slab", "tile", None),
        P(None, "slab", "tile", None),
        P("slab", "tile", None),
        P("slab", None, None, "tile", None),
        P("slab", None, None, None, "tile", None),
    )
    return jax.shard_map(
        step,
        mesh=mesh,
        in_specs=placed,
        out_specs=(
            P(None, "slab", "tile", None),
            P("slab", None, None, "tile", None),
            P("slab", None, None, None, "tile", None),
        ),
        check_vma=False,
    )
```

```python
import functools
import math

import jax
import jax.numpy as jnp
from jax import lax
from jax.experimental import pallas as pl
from jax.experimental.pallas import tpu as pltpu
from jax.sharding import PartitionSpec as P

MESH = pl.DeviceIdType.MESH
TERMS = 4
pade_weights = [2.0 / 9.0 * math.sin(j * math.pi / 9.0) ** 2 for j in range(1, 5)]
pade_decays = [math.cos(j * math.pi / 9.0) ** 2 for j in range(1, 5)]
LANES = 128
PAD = 8
VMEM_TOTAL = 63 * 2**20 + 2**18


PAIRS = 2


def lane_masks():
    lane = lax.broadcasted_iota(jnp.int32, (8, LANES), 1)
    return lane, lane < LANES - 1, lane > 0


def back(value):
    return pltpu.roll(value, LANES - 1, 1)


def forth(value):
    return pltpu.roll(value, 1, 1)


def sweep(src, cur, mg, k, count, r, initial, write):
    cols = src.shape[2]
    top = PAD + 8 * r
    _, not_last, not_first = lane_masks()
    zero_tile = jnp.zeros((8, LANES), jnp.float32)
    loaded = {}

    def at(comp, plane, step_y, c):
        key = (comp, plane, step_y, c)
        if key not in loaded:
            loaded[key] = src[comp, k + 1 + plane, c, pl.ds(top + step_y, 8), :]
        return loaded[key]

    def rise(plane, c):
        key = ("rise", plane, c)
        if key not in loaded:
            loaded[key] = at(2, plane, 1, c) - at(2, plane, 0, c)
        return loaded[key]

    def opening(n, c):
        if c == cols:
            return (zero_tile,) * 3
        ey, ez = at(1, n, 0, c), at(2, n, 0, c)
        t = (ey - at(1, n, -1, c)) + (ez - at(2, n - 1, 0, c))
        loaded["t", n, c] = t
        return back(ey), back(ez), back(t)

    turned = [opening(n, 0) for n in range(count)]
    before = [(zero_tile, zero_tile)] * count
    for c in range(cols):
        for n in range(count):
            turned_there = opening(n, c + 1)
            eyr, ezr, tn = (
                jnp.where(not_last, a, b) for a, b in zip(turned[n], turned_there)
            )
            turned[n] = turned_there
            ey, ez, t = at(1, n, 0, c), at(2, n, 0, c), loaded["t", n, c]
            ex, exjp, exkp = at(0, n, 0, c), at(0, n, 1, c), at(0, n + 1, 0, c)
            hz = (eyr - ey) - (exjp - ex)
            hy = (exkp - ex) - (ezr - ez)
            hz_turned, hy_turned = forth(hz), forth(hy)
            dhz = hz - jnp.where(not_first, hz_turned, before[n][0])
            dhy = hy - jnp.where(not_first, hy_turned, before[n][1])
            before[n] = (hz_turned, hy_turned)
            place = (k + n, pl.ds(8 * r, 8), pl.ds(c * LANES, LANES))
            if initial:
                g = 0.5 / (mg[place] + 4.0)
                mg[place] = g
            else:
                g = mg[place]
            keep = 0.5 + 2.0 * g
            around = (exjp + at(0, n, -1, c)) + (exkp + at(0, n - 1, 0, c))
            new_x = 0.5 * ex + g * ((cur[(0, *place)] + around) - (tn - t))
            eykp = at(1, n + 1, 0, c)
            around = ((eykp + at(1, n - 1, 0, c)) - rise(n, c)) + rise(n - 1, c)
            new_y = keep * ey + g * ((cur[(1, *place)] + around) + dhz)
            around = ((at(2, n, 1, c) + at(2, n, -1, c)) - (eykp - ey)) + (
                at(1, n + 1, -1, c) - at(1, n, -1, c)
            )
            new_z = keep * ez + g * ((cur[(2, *place)] + around) - dhy)
            write(place, (new_x, new_y, new_z), g, c)


def kernel(
    n_slab,
    n_tile,
    electric,
    current,
    mass,
    interface,
    auxiliary,
    smoothed,
    next_if,
    next_aux,
    e1,
    cur,
    mg,
    osum,
    e0,
    ax,
    tr,
    out,
    pu1,
    pd1,
    ru1,
    rd1,
    pua,
    pda,
    rua,
    rda,
    pu2,
    pd2,
    ru2,
    rd2,
    load_sem,
    send_sem,
    recv_sem,
):
    planes, rows, width = electric.shape[1:]
    cols = width // LANES
    tiles = rows // 8
    depth = planes + 2
    tall = rows + 2 * PAD
    pitch = cols * tall
    last = PAD + rows - 1
    inner = tuple(range(1, tiles - 1))
    outer = (0, tiles - 1)
    slab = lax.axis_index("slab")
    tile = lax.axis_index("tile")
    has_up = tile < n_tile - 1
    has_dn = tile > 0
    slab_up = slab < n_slab - 1
    slab_dn = slab > 0
    up = {"tile": tile + 1}
    dn = {"tile": tile - 1}
    sup = {"slab": slab + 1}
    sdn = {"slab": slab - 1}

    def columns(ref, c):
        return ref.at[..., pl.ds(c * LANES, LANES)]

    body = pl.ds(PAD, rows)

    def field_load(c, slot, low, high, row, count):
        return pltpu.make_async_copy(
            electric.at[:, pl.ds(low, high - low), pl.ds(row, count), pl.ds(c * LANES, LANES)],
            e0.at[:, pl.ds(1 + low, high - low), c, pl.ds(PAD + row, count), :],
            load_sem.at[slot, c],
        )

    edge_loads = [field_load(c, 0, 0, planes, 0, 8) for c in range(cols)]
    edge_loads += [field_load(c, 1, 0, planes, rows - 8, 8) for c in range(cols)]

    def cell_loads(slot, low, high, row, count):
        where = (pl.ds(low, high - low), pl.ds(row, count))
        return [
            pltpu.make_async_copy(mass.at[where], mg.at[where], load_sem.at[8, slot]),
            pltpu.make_async_copy(
                current.at[(slice(None), *where)],
                cur.at[(slice(None), *where)],
                load_sem.at[8, slot + 1],
            ),
        ]

    half = 6
    split = half + 2
    loads_a = [field_load(c, 2, 0, split, 8, rows - 16) for c in range(cols)]
    loads_a += cell_loads(0, 0, half, 8, rows - 16)
    loads_b = [field_load(c, 9, split, planes, 8, rows - 16) for c in range(cols)]
    loads_b += cell_loads(2, half, planes, 8, rows - 16)
    outer_loads = cell_loads(4, 0, planes, 0, 8) + cell_loads(6, 0, planes, rows - 8, 8)

    def ghost_loads(buf, slot):
        return [
            pltpu.make_async_copy(
                columns(interface, c).at[0, side],
                buf.at[pl.ds(0, 2), side * (depth - 1), c, body, :],
                load_sem.at[slot + side, c],
            )
            for side in range(2)
            for c in range(cols)
        ]

    ghosts0, ghosts1 = ghost_loads(e0, 3), ghost_loads(e1, 5)
    aux_loads = [
        pltpu.make_async_copy(
            columns(auxiliary, c).at[0], ax.at[:, :, :, c, body, :], load_sem.at[7, c]
        )
        for c in range(cols)
    ]
    for copy in (*edge_loads, *ghosts0):
        copy.start()

    barrier = pltpu.get_barrier_semaphore()
    for there, who in ((has_up, up), (has_dn, dn), (slab_up, sup), (slab_dn, sdn)):

        @pl.when(there)
        def _():
            pl.semaphore_signal(barrier, inc=1, device_id=who, device_id_type=MESH)

    for copy in (*loads_a, *loads_b, *aux_loads, *outer_loads, *ghosts1):
        copy.start()

    def exchange(slot, src_up, dst_up, src_dn, dst_dn):
        goes_up = pltpu.make_async_remote_copy(
            src_ref=src_up,
            dst_ref=dst_up,
            send_sem=send_sem.at[slot, 0],
            recv_sem=recv_sem.at[slot, 0],
            device_id=up,
            device_id_type=MESH,
        )
        goes_dn = pltpu.make_async_remote_copy(
            src_ref=src_dn,
            dst_ref=dst_dn,
            send_sem=send_sem.at[slot, 1],
            recv_sem=recv_sem.at[slot, 1],
            device_id=dn,
            device_id_type=MESH,
        )
        return goes_up, goes_dn

    def part(slot, bufs, at, count):
        return exchange(slot, *(buf.at[pl.ds(at, count)] for buf in bufs))

    def start(pair):
        @pl.when(has_up)
        def _():
            pair[0].start()

        @pl.when(has_dn)
        def _():
            pair[1].start()

    def arrived(pair):
        @pl.when(has_dn)
        def _():
            pair[0].wait_recv()

        @pl.when(has_up)
        def _():
            pair[1].wait_recv()

    def sent(pair):
        @pl.when(has_up)
        def _():
            pair[0].wait_send()

        @pl.when(has_dn)
        def _():
            pair[1].wait_send()

    far = planes - 3
    near1 = ((0, 2, 0), (far, planes, 4))
    rest1 = ((2, far, 10),)
    near2 = ((0, 1, 0), (planes - 2, planes, 2))
    rest2 = ((1, planes - 2, 12),)
    first_near = part(0, (pu1, ru1, pd1, rd1), 0, 10)
    first_rest = part(1, (pu1, ru1, pd1, rd1), 10, 2 * (planes - 5))
    aux_rows = exchange(2, pua, rua, pda, rda)
    second_near = part(3, (pu2, ru2, pd2, rd2), 0, 12)
    second_rest = part(4, (pu2, ru2, pd2, rd2), 12, 2 * (planes - 3))
    slab_goes_up = pltpu.make_async_remote_copy(
        src_ref=out.at[1],
        dst_ref=next_if.at[0, 0],
        send_sem=send_sem.at[5, 0],
        recv_sem=recv_sem.at[5, 0],
        device_id=sup,
        device_id_type=MESH,
    )
    slab_goes_dn = pltpu.make_async_remote_copy(
        src_ref=out.at[0],
        dst_ref=next_if.at[0, 1],
        send_sem=send_sem.at[5, 1],
        recv_sem=recv_sem.at[5, 1],
        device_id=sdn,
        device_id_type=MESH,
    )

    flat0 = e0.reshape(3 * depth * pitch, LANES)
    flat1 = e1.reshape(3 * depth * pitch, LANES)
    flata = ax.reshape(2 * TERMS * 2 * pitch, LANES)
    flatt = tr.reshape(6 * pitch, LANES)
    zero_row = jnp.zeros((cols, LANES), jnp.float32)
    zero_tile = jnp.zeros((8, LANES), jnp.float32)

    def line(plane, row):
        return pl.ds(plane * pitch + row, cols, stride=tall)

    for buf in (e0, e1):
        for c in range(cols):
            for r in range(tall // 8):
                buf[2, 0, c, pl.ds(8 * r, 8), :] = zero_tile

    @pl.loop(1, depth)
    def _(p):
        for flat in (flat0, flat1):
            for comp in range(3):
                flat[line(comp * depth + p, PAD - 1), :] = zero_row
            for comp in (0, 2):
                flat[line(comp * depth + p, last + 1), :] = zero_row

    @pl.loop(0, 2 * TERMS * 2)
    def _(p):
        flata[line(p, PAD - 1), :] = zero_row
        flata[line(p, last + 1), :] = zero_row

    for p in range(4):
        flatt[line(p, PAD - 1), :] = zero_row
        flatt[line(p, last + 1), :] = zero_row

    @pl.when(jnp.logical_not(slab_dn))
    def _():
        next_if[0, 0] = jnp.zeros(next_if.shape[2:], jnp.float32)

    @pl.when(jnp.logical_not(slab_up))
    def _():
        next_if[0, 1] = jnp.zeros(next_if.shape[2:], jnp.float32)

    lane, not_last, not_first = lane_masks()
    sub = lax.broadcasted_iota(jnp.int32, (cols, LANES), 0)
    row_lane = lax.broadcasted_iota(jnp.int32, (cols, LANES), 1)

    def row_ahead(row):
        turned = pltpu.roll(row, LANES - 1, 1)
        wrapped = jnp.where(sub < cols - 1, pltpu.roll(turned, cols - 1, 0), 0.0)
        return jnp.where(row_lane < LANES - 1, turned, wrapped)

    def row_behind(row):
        turned = pltpu.roll(row, 1, 1)
        wrapped = jnp.where(sub > 0, pltpu.roll(turned, 1, 0), 0.0)
        return jnp.where(row_lane > 0, turned, wrapped)

    def pack(flat, to_up, to_dn, spans):
        for low, high, at in spans:

            @pl.loop(low, high)
            def _(k):
                spot = at + PAIRS * (k - low)
                ey = flat[line(depth + 1 + k, last), :]
                over = flat[line(depth + 2 + k, last), :]
                to_up[spot] = (row_ahead(ey) - ey) + flat[line(1 + k, last), :]
                to_up[spot + 1] = flat[line(2 * depth + 1 + k, last), :] + (over - ey)
                to_dn[spot] = flat[line(1 + k, PAD), :]
                to_dn[spot + 1] = flat[line(2 * depth + 1 + k, PAD), :]

    def unpack(flat, from_dn, from_up, spans):
        for there, source, row in ((has_dn, from_dn, PAD - 1), (has_up, from_up, last + 1)):

            @pl.when(there)
            def _():
                for low, high, at in spans:

                    @pl.loop(low, high)
                    def _(k):
                        spot = at + PAIRS * (k - low)
                        flat[line(1 + k, row), :] = source[spot]
                        flat[line(2 * depth + 1 + k, row), :] = source[spot + 1]

    def first_sweep(which, start_at, steps, stride=2):
        @pl.loop(0, steps)
        def _(step):
            k = start_at + stride * step
            for r in which:

                def write(place, news, g, c):
                    for comp in range(3):
                        e1[comp, place[0] + 1, c, pl.ds(PAD + 8 * r, 8), :] = news[comp]

                sweep(e0, cur, mg, k, 2, r, True, write)

    def second_sweep_inner(start_at, steps):
        @pl.loop(0, steps)
        def _(step):
            for r in inner:

                def write(place, news, g, c):
                    for comp in range(3):
                        smoothed[(comp, *place)] = news[comp]

                sweep(e1, cur, mg, start_at + 2 * step, 2, r, False, write)

    def second_sweep_ends(which):
        @pl.loop(0, 2)
        def _(side):
            k = side * (planes - 1)
            for r in which:

                def write(place, news, g, c):
                    for comp in range(3):
                        smoothed[(comp, *place)] = news[comp]
                    for comp in range(2):
                        tr[side * 2 + comp, c, pl.ds(PAD + 8 * r, 8), :] = news[comp]
                    tr[4 + side, c, pl.ds(PAD + 8 * r, 8), :] = g

                sweep(e1, cur, mg, k, 1, r, False, write)

    edge_last = jnp.where(lane == LANES - 1, 3.0, 4.0)
    edge_first = jnp.where(lane == 0, 3.0, 4.0)

    def surface(read, comp, r, scale, write):
        top = PAD + 8 * r
        u = read(0, top)
        turned, before = back(u), zero_tile
        for c in range(cols):
            if c + 1 < cols:
                u_there = read(c + 1, top)
                turned_there = back(u_there)
            else:
                u_there, turned_there = None, zero_tile
            after = jnp.where(not_last, turned, turned_there)
            fore = forth(u)
            behind = jnp.where(not_first, fore, before)
            if comp == 0 and c == cols - 1:
                centre = (edge_last * (scale / 8)) * u
            elif comp == 1 and c == 0:
                centre = (edge_first * (scale / 8)) * u
            else:
                centre = (scale / 2) * u
            around = (after + behind) + (read(c, top + 1) + read(c, top - 1))
            write(c, u, centre - (scale / 8) * around)
            u, turned, before = u_there, turned_there, fore

    def aux_surface(which):
        @pl.loop(0, 2)
        def _(side):
            for comp in range(2):
                for r in which:
                    for j in range(TERMS):

                        def read(c, row):
                            return ax[side, j, comp, c, pl.ds(row, 8), :]

                        def write(c, u, image):
                            place = (pl.ds(8 * r, 8), pl.ds(c * LANES, LANES))
                            next_aux[(0, side, j, comp, *place)] = image
                            total = pade_weights[j] * image
                            if j:
                                total = osum[(side, comp, *place)] + total
                            osum[(side, comp, *place)] = total

                        surface(read, comp, r, pade_decays[j], write)

    for copy in (*edge_loads, *ghosts0):
        copy.wait()
    pack(flat0, pu1, pd1, near1)

    peers = sum(jnp.where(there, 1, 0) for there in (has_up, has_dn, slab_up, slab_dn))
    pl.semaphore_wait(barrier, peers)
    start(first_near)
    pack(flat0, pu1, pd1, rest1)
    start(first_rest)

    for copy in loads_a:
        copy.wait()
    first_sweep(inner, 0, half // 2)
    for copy in loads_b:
        copy.wait()
    first_sweep(inner, half, (planes - half) // 2)
    for copy in aux_loads:
        copy.wait()

    @pl.loop(0, 2 * TERMS * 2)
    def _(p):
        pua[p] = flata[line(p, last), :]
        pda[p] = flata[line(p, PAD), :]

    start(aux_rows)
    aux_surface(inner)
    for copy in (*outer_loads, *ghosts1):
        copy.wait()
    arrived(first_near)
    unpack(flat0, ru1, rd1, near1)
    first_sweep(outer, 0, 2, planes - 2)

    second_sweep_ends(outer)
    pack(flat1, pu2, pd2, near2)
    for p in range(6):
        pu2[6 + p] = flatt[line(p, last), :]
        pd2[6 + p] = flatt[line(p, PAD), :]
    start(second_near)

    arrived(first_rest)
    unpack(flat0, ru1, rd1, rest1)
    first_sweep(outer, 2, (planes - 4) // 2)
    pack(flat1, pu2, pd2, rest2)
    start(second_rest)

    second_sweep_ends(inner)
    arrived(aux_rows)
    for there, source, row in ((has_dn, rua, PAD - 1), (has_up, rda, last + 1)):

        @pl.when(there)
        def _():
            @pl.loop(0, 2 * TERMS * 2)
            def _(p):
                flata[line(p, row), :] = source[p]

    aux_surface(outer)

    arrived(second_near)
    unpack(flat1, ru2, rd2, near2)

    @pl.when(has_dn)
    def _():
        for side, (x, z, z_below) in enumerate(((0, 1, None), (4, 5, 3))):
            g = ru2[10 + side]
            row = pd2[x]
            slope = row - row_behind(row) + pd2[z]
            if z_below is not None:
                slope = slope - pd2[z_below]
            flatt[line(2 * side, PAD - 1), :] = ru2[6 + 2 * side] + g * row
            flatt[line(2 * side + 1, PAD - 1), :] = ru2[7 + 2 * side] - g * slope

    @pl.when(has_up)
    def _():
        for side, x in enumerate((0, 4)):
            g = rd2[10 + side]
            flatt[line(2 * side, last + 1), :] = rd2[6 + 2 * side] + g * pu2[x]
            flatt[line(2 * side + 1, last + 1), :] = rd2[7 + 2 * side]

    second_sweep_ends(outer)
    weight = sum(pade_weights)

    @pl.loop(0, 2)
    def _(side):
        for comp in range(2):
            for r in range(tiles):

                def read(c, row):
                    return tr[side * 2 + comp, c, pl.ds(row, 8), :]

                def write(c, u, image):
                    place = (side, comp, pl.ds(8 * r, 8), pl.ds(c * LANES, LANES))
                    out[place] = (u + weight * image) - osum[place]
                    osum[place] = image

                surface(read, comp, r, 1.0, write)

    @pl.when(slab_up)
    def _():
        slab_goes_up.start()

    @pl.when(slab_dn)
    def _():
        slab_goes_dn.start()

    second_sweep_inner(1, planes // 2 - 1)
    arrived(second_rest)
    unpack(flat1, ru2, rd2, rest2)

    for pair in (first_near, first_rest, aux_rows, second_near, second_rest):
        sent(pair)

    @pl.when(slab_dn)
    def _():
        slab_goes_up.wait_recv()
        slab_goes_dn.wait_send()

    @pl.when(slab_up)
    def _():
        slab_goes_dn.wait_recv()
        slab_goes_up.wait_send()


def store_kernel(
    field, face, aux, e1, cur, mg, osum, field_out, face_out, aux_out, rim, aux_held, sem, rim_sem
):
    _, planes, rows, width = field.shape
    cols = width // LANES
    outer = (0, rows // 8 - 1)
    places = [(comp, slice(1, planes - 1), pl.ds(8, rows - 16)) for comp in range(3)]
    places += [(slice(None), k) for k in (0, planes - 1)]
    stores = [
        pltpu.make_async_copy(field.at[place], field_out.at[place], sem.at[i])
        for i, place in enumerate(places)
    ]
    stores.append(pltpu.make_async_copy(face, face_out, sem.at[5]))
    for copy in stores:
        copy.start()

    def aux_store(side):
        return pltpu.make_async_copy(aux_held.at[side], aux_out.at[0, side], sem.at[6 + side])

    for side in range(2):

        @pl.loop(0, 2)
        def _(comp):
            for r in range(rows // 8):
                for c in range(cols):
                    place = (comp, pl.ds(8 * r, 8), pl.ds(c * LANES, LANES))
                    image = osum[(side, *place)]
                    for j in range(TERMS):
                        aux_held[(side, j, *place)] = image - aux[(0, side, j, *place)]

        aux_store(side).start()

    def rim_store(step, i):
        return pltpu.make_async_copy(
            rim.at[i, :, pl.ds(2 * step, 2)],
            field_out.at[:, pl.ds(1 + 2 * step, 2), pl.ds(8 * outer[i], 8)],
            rim_sem.at[i, step],
        )

    steps = planes // 2 - 1

    @pl.loop(0, steps)
    def _(step):
        for i, r in enumerate(outer):

            def write(place, news, g, c):
                for comp in range(3):
                    rim[i, comp, place[0] - 1, :, pl.ds(c * LANES, LANES)] = news[comp]

            sweep(e1, cur, mg, 1 + 2 * step, 2, r, False, write)
            rim_store(step, i).start()

    for copy in (*stores, aux_store(0), aux_store(1)):
        copy.wait()

    @pl.loop(0, steps)
    def _(step):
        for i in range(2):
            rim_store(step, i).wait()


def solution(mesh):
    n_slab, n_tile = mesh.shape["slab"], mesh.shape["tile"]

    def step(electric, current, mass_shift, interface, auxiliary):
        _, planes, rows, width = electric.shape
        cols = width // LANES
        tall = rows + 2 * PAD
        f32 = jnp.float32
        hbm = pl.BlockSpec(memory_space=pltpu.MemorySpace.HBM)
        vmem = pl.BlockSpec(memory_space=pltpu.VMEM)
        shapes = (electric.shape, interface.shape, auxiliary.shape)
        padded = (3, planes + 2, cols, tall, LANES)
        faces = (2, 2, rows, width)
        held_shapes = (*shapes, padded, electric.shape, mass_shift.shape, faces)
        held_bytes = sum(4 * math.prod(shape) for shape in held_shapes)

        def lines(n):
            return pltpu.VMEM((n, cols, LANES), f32)

        held = pl.pallas_call(
            functools.partial(kernel, n_slab, n_tile),
            out_shape=tuple(pltpu.VMEM(shape, f32) for shape in held_shapes),
            in_specs=[hbm] * 5,
            out_specs=(vmem,) * 7,
            scratch_shapes=[
                pltpu.VMEM(padded, f32),
                pltpu.VMEM((2, TERMS, 2, cols, tall, LANES), f32),
                pltpu.VMEM((6, cols, tall, LANES), f32),
                pltpu.VMEM(faces, f32),
                *[lines(2 * planes)] * 4,
                *[lines(4 * TERMS)] * 4,
                *[lines(2 * planes + 6)] * 4,
                pltpu.SemaphoreType.DMA((10, cols)),
                pltpu.SemaphoreType.DMA((6, 2)),
                pltpu.SemaphoreType.DMA((6, 2)),
            ],
            compiler_params=pltpu.CompilerParams(
                collective_id=0,
                has_side_effects=True,
                vmem_limit_bytes=VMEM_TOTAL - held_bytes,
            ),
        )(electric, current, mass_shift, interface, auxiliary)
        return pl.pallas_call(
            store_kernel,
            out_shape=tuple(jax.ShapeDtypeStruct(shape, f32) for shape in shapes),
            in_specs=[vmem] * 7,
            out_specs=(hbm, hbm, hbm),
            scratch_shapes=[
                pltpu.VMEM((2, 3, planes - 2, 8, width), f32),
                pltpu.VMEM((2, TERMS, 2, rows, width), f32),
                pltpu.SemaphoreType.DMA((8,)),
                pltpu.SemaphoreType.DMA((2, planes // 2 - 1)),
            ],
            compiler_params=pltpu.CompilerParams(
                vmem_limit_bytes=8 * 2**20
            ),
        )(*held)

    placed = (
        P(None, "slab", "tile", None),
        P(None, "slab", "tile", None),
        P("slab", "tile", None),
        P("slab", None, None, "tile", None),
        P("slab", None, None, None, "tile", None),
    )
    return jax.shard_map(
        step,
        mesh=mesh,
        in_specs=placed,
        out_specs=(
            P(None, "slab", "tile", None),
            P("slab", None, None, "tile", None),
            P("slab", None, None, None, "tile", None),
        ),
        check_vma=False,
    )
```

```python
import functools
import math

import jax
import jax.numpy as jnp
from jax import lax
from jax.experimental import pallas as pl
from jax.experimental.pallas import tpu as pltpu
from jax.sharding import PartitionSpec as P

MESH = pl.DeviceIdType.MESH
TERMS = 4
pade_weights = [2.0 / 9.0 * math.sin(j * math.pi / 9.0) ** 2 for j in range(1, 5)]
pade_decays = [math.cos(j * math.pi / 9.0) ** 2 for j in range(1, 5)]
LANES = 128
PAD = 8
VMEM_TOTAL = 63 * 2**20 + 2**18


PAIRS = 2


def lane_masks():
    lane = lax.broadcasted_iota(jnp.int32, (8, LANES), 1)
    return lane, lane < LANES - 1, lane > 0


def back(value):
    return pltpu.roll(value, LANES - 1, 1)


def forth(value):
    return pltpu.roll(value, 1, 1)


def sweep(src, cur, mg, k, count, r, initial, write):
    cols = src.shape[2]
    top = PAD + 8 * r
    _, not_last, not_first = lane_masks()
    zero_tile = jnp.zeros((8, LANES), jnp.float32)
    loaded = {}

    def at(comp, plane, step_y, c):
        key = (comp, plane, step_y, c)
        if key not in loaded:
            loaded[key] = src[comp, k + 1 + plane, c, pl.ds(top + step_y, 8), :]
        return loaded[key]

    def rise(plane, c):
        key = ("rise", plane, c)
        if key not in loaded:
            loaded[key] = at(2, plane, 1, c) - at(2, plane, 0, c)
        return loaded[key]

    def opening(n, c):
        if c == cols:
            return (zero_tile,) * 3
        ey, ez = at(1, n, 0, c), at(2, n, 0, c)
        t = (ey - at(1, n, -1, c)) + (ez - at(2, n - 1, 0, c))
        loaded["t", n, c] = t
        return back(ey), back(ez), back(t)

    turned = [opening(n, 0) for n in range(count)]
    before = [(zero_tile, zero_tile)] * count
    for c in range(cols):
        for n in range(count):
            turned_there = opening(n, c + 1)
            eyr, ezr, tn = (
                jnp.where(not_last, a, b) for a, b in zip(turned[n], turned_there)
            )
            turned[n] = turned_there
            ey, ez, t = at(1, n, 0, c), at(2, n, 0, c), loaded["t", n, c]
            ex, exjp, exkp = at(0, n, 0, c), at(0, n, 1, c), at(0, n + 1, 0, c)
            hz = (eyr - ey) - (exjp - ex)
            hy = (exkp - ex) - (ezr - ez)
            hz_turned, hy_turned = forth(hz), forth(hy)
            dhz = hz - jnp.where(not_first, hz_turned, before[n][0])
            dhy = hy - jnp.where(not_first, hy_turned, before[n][1])
            before[n] = (hz_turned, hy_turned)
            place = (k + n, pl.ds(8 * r, 8), pl.ds(c * LANES, LANES))
            if initial:
                g = 0.5 / (mg[place] + 4.0)
                mg[place] = g
            else:
                g = mg[place]
            keep = 0.5 + 2.0 * g
            around = (exjp + at(0, n, -1, c)) + (exkp + at(0, n - 1, 0, c))
            new_x = 0.5 * ex + g * ((cur[(0, *place)] + around) - (tn - t))
            eykp = at(1, n + 1, 0, c)
            around = ((eykp + at(1, n - 1, 0, c)) - rise(n, c)) + rise(n - 1, c)
            new_y = keep * ey + g * ((cur[(1, *place)] + around) + dhz)
            around = ((at(2, n, 1, c) + at(2, n, -1, c)) - (eykp - ey)) + (
                at(1, n + 1, -1, c) - at(1, n, -1, c)
            )
            new_z = keep * ez + g * ((cur[(2, *place)] + around) - dhy)
            write(place, (new_x, new_y, new_z), g, c)


def kernel(
    n_slab,
    n_tile,
    electric,
    current,
    mass,
    interface,
    auxiliary,
    smoothed,
    next_if,
    next_aux,
    e1,
    cur,
    mg,
    osum,
    e0,
    ax,
    tr,
    sb,
    out,
    pu1,
    pd1,
    ru1,
    rd1,
    pua,
    pda,
    rua,
    rda,
    pu2,
    pd2,
    ru2,
    rd2,
    load_sem,
    send_sem,
    recv_sem,
):
    planes, rows, width = electric.shape[1:]
    cols = width // LANES
    tiles = rows // 8
    depth = planes + 2
    tall = rows + 2 * PAD
    pitch = cols * tall
    last = PAD + rows - 1
    inner = tuple(range(1, tiles - 1))
    outer = (0, tiles - 1)
    slab = lax.axis_index("slab")
    tile = lax.axis_index("tile")
    has_up = tile < n_tile - 1
    has_dn = tile > 0
    slab_up = slab < n_slab - 1
    slab_dn = slab > 0
    up = {"tile": tile + 1}
    dn = {"tile": tile - 1}
    sup = {"slab": slab + 1}
    sdn = {"slab": slab - 1}

    def columns(ref, c):
        return ref.at[..., pl.ds(c * LANES, LANES)]

    body = pl.ds(PAD, rows)

    def field_load(c, slot, low, high, row, count):
        return pltpu.make_async_copy(
            electric.at[:, pl.ds(low, high - low), pl.ds(row, count), pl.ds(c * LANES, LANES)],
            e0.at[:, pl.ds(1 + low, high - low), c, pl.ds(PAD + row, count), :],
            load_sem.at[slot, c],
        )

    edge_loads = [field_load(c, 0, 0, planes, 0, 8) for c in range(cols)]
    edge_loads += [field_load(c, 1, 0, planes, rows - 8, 8) for c in range(cols)]

    def cell_loads(slot, low, high, row, count):
        where = (pl.ds(low, high - low), pl.ds(row, count))
        return [
            pltpu.make_async_copy(mass.at[where], mg.at[where], load_sem.at[8, slot]),
            pltpu.make_async_copy(
                current.at[(slice(None), *where)],
                cur.at[(slice(None), *where)],
                load_sem.at[8, slot + 1],
            ),
        ]

    half = 6
    split = half + 2
    loads_a = [field_load(c, 2, 0, split, 8, rows - 16) for c in range(cols)]
    loads_a += cell_loads(0, 0, half, 8, rows - 16)
    loads_b = [field_load(c, 9, split, planes, 8, rows - 16) for c in range(cols)]
    loads_b += cell_loads(2, half, planes, 8, rows - 16)
    outer_loads = cell_loads(4, 0, planes, 0, 8) + cell_loads(6, 0, planes, rows - 8, 8)

    def ghost_loads(buf, slot):
        return [
            pltpu.make_async_copy(
                columns(interface, c).at[0, side],
                buf.at[pl.ds(0, 2), side * (depth - 1), c, body, :],
                load_sem.at[slot + side, c],
            )
            for side in range(2)
            for c in range(cols)
        ]

    ghosts0, ghosts1 = ghost_loads(e0, 3), ghost_loads(e1, 5)
    aux_loads = [
        pltpu.make_async_copy(
            columns(auxiliary, c).at[0], ax.at[:, :, :, c, body, :], load_sem.at[7, c]
        )
        for c in range(cols)
    ]
    for copy in (*edge_loads, *ghosts0):
        copy.start()

    barrier = pltpu.get_barrier_semaphore()
    for there, who in ((has_up, up), (has_dn, dn), (slab_up, sup), (slab_dn, sdn)):

        @pl.when(there)
        def _():
            pl.semaphore_signal(barrier, inc=1, device_id=who, device_id_type=MESH)

    def exchange(slot, src_up, dst_up, src_dn, dst_dn):
        goes_up = pltpu.make_async_remote_copy(
            src_ref=src_up,
            dst_ref=dst_up,
            send_sem=send_sem.at[slot, 0],
            recv_sem=recv_sem.at[slot, 0],
            device_id=up,
            device_id_type=MESH,
        )
        goes_dn = pltpu.make_async_remote_copy(
            src_ref=src_dn,
            dst_ref=dst_dn,
            send_sem=send_sem.at[slot, 1],
            recv_sem=recv_sem.at[slot, 1],
            device_id=dn,
            device_id_type=MESH,
        )
        return goes_up, goes_dn

    def part(slot, bufs, at, count):
        return exchange(slot, *(buf.at[pl.ds(at, count)] for buf in bufs))

    def start(pair):
        @pl.when(has_up)
        def _():
            pair[0].start()

        @pl.when(has_dn)
        def _():
            pair[1].start()

    def arrived(pair):
        @pl.when(has_dn)
        def _():
            pair[0].wait_recv()

        @pl.when(has_up)
        def _():
            pair[1].wait_recv()

    def sent(pair):
        @pl.when(has_up)
        def _():
            pair[0].wait_send()

        @pl.when(has_dn)
        def _():
            pair[1].wait_send()

    far = planes - 3
    near1 = ((0, 2, 0), (far, planes, 4))
    rest1 = ((2, far, 10),)
    near2 = ((0, 1, 0), (planes - 2, planes, 2))
    rest2 = ((1, planes - 2, 16),)
    first_near = part(0, (pu1, ru1, pd1, rd1), 0, 10)
    first_rest = part(1, (pu1, ru1, pd1, rd1), 10, 2 * (planes - 5))
    aux_rows = exchange(2, pua, rua, pda, rda)
    second_near = part(3, (pu2, ru2, pd2, rd2), 0, 16)
    second_rest = part(4, (pu2, ru2, pd2, rd2), 16, 2 * (planes - 3))
    def slab_part(slot, row, count):
        goes_up = pltpu.make_async_remote_copy(
            src_ref=out.at[1, :, pl.ds(row, count)],
            dst_ref=next_if.at[0, 0, :, pl.ds(row, count)],
            send_sem=send_sem.at[slot, 0],
            recv_sem=recv_sem.at[slot, 0],
            device_id=sup,
            device_id_type=MESH,
        )
        goes_dn = pltpu.make_async_remote_copy(
            src_ref=out.at[0, :, pl.ds(row, count)],
            dst_ref=next_if.at[0, 1, :, pl.ds(row, count)],
            send_sem=send_sem.at[slot, 1],
            recv_sem=recv_sem.at[slot, 1],
            device_id=sdn,
            device_id_type=MESH,
        )
        return goes_up, goes_dn

    slab_inner = slab_part(5, 8, rows - 16)
    slab_outer = (slab_part(6, 0, 8), slab_part(7, rows - 8, 8))

    def slab_start(parts):
        @pl.when(slab_up)
        def _():
            for goes_up, _ in parts:
                goes_up.start()

        @pl.when(slab_dn)
        def _():
            for _, goes_dn in parts:
                goes_dn.start()

    flat0 = e0.reshape(3 * depth * pitch, LANES)
    flat1 = e1.reshape(3 * depth * pitch, LANES)
    flata = ax.reshape(2 * TERMS * 2 * pitch, LANES)
    flatt = tr.reshape(6 * pitch, LANES)
    flats = sb.reshape(4 * pitch, LANES)
    zero_row = jnp.zeros((cols, LANES), jnp.float32)
    zero_tile = jnp.zeros((8, LANES), jnp.float32)

    def line(plane, row):
        return pl.ds(plane * pitch + row, cols, stride=tall)

    for buf in (e0, e1):
        for c in range(cols):
            for r in range(tall // 8):
                buf[2, 0, c, pl.ds(8 * r, 8), :] = zero_tile

    @pl.loop(1, depth)
    def _(p):
        for flat in (flat0, flat1):
            for comp in range(3):
                flat[line(comp * depth + p, PAD - 1), :] = zero_row
            for comp in (0, 2):
                flat[line(comp * depth + p, last + 1), :] = zero_row

    @pl.loop(0, 2 * TERMS * 2)
    def _(p):
        flata[line(p, PAD - 1), :] = zero_row
        flata[line(p, last + 1), :] = zero_row

    for p in range(4):
        for flat in (flatt, flats):
            flat[line(p, PAD - 1), :] = zero_row
            flat[line(p, last + 1), :] = zero_row

    @pl.when(jnp.logical_not(slab_dn))
    def _():
        next_if[0, 0] = jnp.zeros(next_if.shape[2:], jnp.float32)

    @pl.when(jnp.logical_not(slab_up))
    def _():
        next_if[0, 1] = jnp.zeros(next_if.shape[2:], jnp.float32)

    lane, not_last, not_first = lane_masks()
    sub = lax.broadcasted_iota(jnp.int32, (cols, LANES), 0)
    row_lane = lax.broadcasted_iota(jnp.int32, (cols, LANES), 1)

    def row_ahead(row):
        turned = pltpu.roll(row, LANES - 1, 1)
        wrapped = jnp.where(sub < cols - 1, pltpu.roll(turned, cols - 1, 0), 0.0)
        return jnp.where(row_lane < LANES - 1, turned, wrapped)

    def row_behind(row):
        turned = pltpu.roll(row, 1, 1)
        wrapped = jnp.where(sub > 0, pltpu.roll(turned, 1, 0), 0.0)
        return jnp.where(row_lane > 0, turned, wrapped)

    def pack(flat, to_up, to_dn, spans):
        for low, high, at in spans:

            @pl.loop(low, high)
            def _(k):
                spot = at + PAIRS * (k - low)
                ey = flat[line(depth + 1 + k, last), :]
                over = flat[line(depth + 2 + k, last), :]
                to_up[spot] = (row_ahead(ey) - ey) + flat[line(1 + k, last), :]
                to_up[spot + 1] = flat[line(2 * depth + 1 + k, last), :] + (over - ey)
                to_dn[spot] = flat[line(1 + k, PAD), :]
                to_dn[spot + 1] = flat[line(2 * depth + 1 + k, PAD), :]

    def unpack(flat, from_dn, from_up, spans):
        for there, source, row in ((has_dn, from_dn, PAD - 1), (has_up, from_up, last + 1)):

            @pl.when(there)
            def _():
                for low, high, at in spans:

                    @pl.loop(low, high)
                    def _(k):
                        spot = at + PAIRS * (k - low)
                        flat[line(1 + k, row), :] = source[spot]
                        flat[line(2 * depth + 1 + k, row), :] = source[spot + 1]

    def first_sweep(which, start_at, steps, stride=2):
        @pl.loop(0, steps)
        def _(step):
            k = start_at + stride * step
            for r in which:

                def write(place, news, g, c):
                    for comp in range(3):
                        e1[comp, place[0] + 1, c, pl.ds(PAD + 8 * r, 8), :] = news[comp]

                sweep(e0, cur, mg, k, 2, r, True, write)

    def second_sweep_inner(start_at, steps):
        @pl.loop(0, steps)
        def _(step):
            for r in inner:

                def write(place, news, g, c):
                    for comp in range(3):
                        smoothed[(comp, *place)] = news[comp]

                sweep(e1, cur, mg, start_at + 2 * step, 2, r, False, write)

    def second_sweep_ends(which):
        @pl.loop(0, 2)
        def _(side):
            k = side * (planes - 1)
            for r in which:

                def write(place, news, g, c):
                    for comp in range(3):
                        smoothed[(comp, *place)] = news[comp]
                    for comp in range(2):
                        tr[side * 2 + comp, c, pl.ds(PAD + 8 * r, 8), :] = news[comp]
                    tr[4 + side, c, pl.ds(PAD + 8 * r, 8), :] = g

                sweep(e1, cur, mg, k, 1, r, False, write)

    edge_last = jnp.where(lane == LANES - 1, 3.0, 4.0)
    edge_first = jnp.where(lane == 0, 3.0, 4.0)

    def surface(read, comp, r, scale, write):
        top = PAD + 8 * r
        u = read(0, top)
        turned, before = back(u), zero_tile
        for c in range(cols):
            if c + 1 < cols:
                u_there = read(c + 1, top)
                turned_there = back(u_there)
            else:
                u_there, turned_there = None, zero_tile
            after = jnp.where(not_last, turned, turned_there)
            fore = forth(u)
            behind = jnp.where(not_first, fore, before)
            if comp == 0 and c == cols - 1:
                centre = (edge_last * (scale / 8)) * u
            elif comp == 1 and c == 0:
                centre = (edge_first * (scale / 8)) * u
            else:
                centre = (scale / 2) * u
            around = (after + behind) + (read(c, top + 1) + read(c, top - 1))
            write(c, u, centre - (scale / 8) * around)
            u, turned, before = u_there, turned_there, fore

    def aux_surface(which):
        @pl.loop(0, 2)
        def _(side):
            for comp in range(2):
                for r in which:
                    for j in range(TERMS):

                        def read(c, row):
                            return ax[side, j, comp, c, pl.ds(row, 8), :]

                        def write(c, u, image):
                            place = (pl.ds(8 * r, 8), pl.ds(c * LANES, LANES))
                            next_aux[(0, side, j, comp, *place)] = image

                        surface(read, comp, r, pade_decays[j], write)

    weight = sum(pade_weights)

    def weighted_aux():
        @pl.loop(0, 2)
        def _(side):
            for comp in range(2):
                for c in range(cols):
                    for r in range(tiles):
                        place = (comp, c, pl.ds(PAD + 8 * r, 8), slice(None))
                        total = (pade_weights[0] * pade_decays[0] / weight) * ax[(side, 0, *place)]
                        for j in range(1, TERMS):
                            part = pade_weights[j] * pade_decays[j] / weight
                            total = total + part * ax[(side, j, *place)]
                        sb[side * 2 + comp, c, pl.ds(PAD + 8 * r, 8), :] = total

    def outgoing(which):
        @pl.loop(0, 2)
        def _(side):
            for comp in range(2):
                for r in which:

                    def read(c, row):
                        where = (side * 2 + comp, c, pl.ds(row, 8), slice(None))
                        return tr[where] - sb[where]

                    def write(c, u, image):
                        place = (side, comp, pl.ds(8 * r, 8), pl.ds(c * LANES, LANES))
                        out[place] = tr[side * 2 + comp, c, pl.ds(PAD + 8 * r, 8), :] + image

                    surface(read, comp, r, weight, write)

    def trace_surface():
        @pl.loop(0, 2)
        def _(side):
            for comp in range(2):
                for r in range(tiles):

                    def read(c, row):
                        return tr[side * 2 + comp, c, pl.ds(row, 8), :]

                    def write(c, u, image):
                        place = (side, comp, pl.ds(8 * r, 8), pl.ds(c * LANES, LANES))
                        osum[place] = image

                    surface(read, comp, r, 1.0, write)

    for copy in (*edge_loads, *ghosts0):
        copy.wait()
    for copy in loads_a:
        copy.start()
    pack(flat0, pu1, pd1, near1)

    peers = sum(jnp.where(there, 1, 0) for there in (has_up, has_dn, slab_up, slab_dn))
    pl.semaphore_wait(barrier, peers)
    start(first_near)
    for copy in (*loads_b, *aux_loads, *outer_loads, *ghosts1):
        copy.start()
    pack(flat0, pu1, pd1, rest1)
    start(first_rest)

    for copy in loads_a:
        copy.wait()
    first_sweep(inner, 0, half // 2)
    for copy in loads_b:
        copy.wait()
    first_sweep(inner, half, (planes - half) // 2)
    for copy in (*aux_loads, *outer_loads, *ghosts1):
        copy.wait()
    @pl.loop(0, 2 * TERMS * 2)
    def _(p):
        pua[p] = flata[line(p, last), :]
        pda[p] = flata[line(p, PAD), :]

    start(aux_rows)
    weighted_aux()

    arrived(first_near)
    unpack(flat0, ru1, rd1, near1)
    first_sweep(outer, 0, 2, planes - 2)

    second_sweep_ends(outer)
    pack(flat1, pu2, pd2, near2)
    for at, flat, count in ((6, flatt, 6), (12, flats, 4)):
        for p in range(count):
            pu2[at + p] = flat[line(p, last), :]
            pd2[at + p] = flat[line(p, PAD), :]
    start(second_near)

    arrived(first_rest)
    unpack(flat0, ru1, rd1, rest1)
    first_sweep(outer, 2, (planes - 4) // 2)
    pack(flat1, pu2, pd2, rest2)
    start(second_rest)

    second_sweep_ends(inner)
    outgoing(inner)
    slab_start((slab_inner,))
    aux_surface(inner)
    arrived(aux_rows)
    for there, source, row in ((has_dn, rua, PAD - 1), (has_up, rda, last + 1)):

        @pl.when(there)
        def _():
            @pl.loop(0, 2 * TERMS * 2)
            def _(p):
                flata[line(p, row), :] = source[p]

    aux_surface(outer)

    arrived(second_near)
    unpack(flat1, ru2, rd2, near2)

    @pl.when(has_dn)
    def _():
        for side, (x, z, z_below) in enumerate(((0, 1, None), (4, 5, 3))):
            g = ru2[10 + side]
            row = pd2[x]
            slope = row - row_behind(row) + pd2[z]
            if z_below is not None:
                slope = slope - pd2[z_below]
            flatt[line(2 * side, PAD - 1), :] = ru2[6 + 2 * side] + g * row
            flatt[line(2 * side + 1, PAD - 1), :] = ru2[7 + 2 * side] - g * slope
        for p in range(4):
            flats[line(p, PAD - 1), :] = ru2[12 + p]

    @pl.when(has_up)
    def _():
        for side, x in enumerate((0, 4)):
            g = rd2[10 + side]
            flatt[line(2 * side, last + 1), :] = rd2[6 + 2 * side] + g * pu2[x]
            flatt[line(2 * side + 1, last + 1), :] = rd2[7 + 2 * side]
        for p in range(4):
            flats[line(p, last + 1), :] = rd2[12 + p]

    second_sweep_ends(outer)
    outgoing(outer)
    slab_start(slab_outer)

    second_sweep_inner(1, planes // 2 - 1)
    trace_surface()
    arrived(second_rest)
    unpack(flat1, ru2, rd2, rest2)

    for pair in (first_near, first_rest, aux_rows, second_near, second_rest):
        sent(pair)

    @pl.when(slab_dn)
    def _():
        for goes_up, goes_dn in (slab_inner, *slab_outer):
            goes_up.wait_recv()
            goes_dn.wait_send()

    @pl.when(slab_up)
    def _():
        for goes_up, goes_dn in (slab_inner, *slab_outer):
            goes_dn.wait_recv()
            goes_up.wait_send()


def store_kernel(
    field, face, aux, e1, cur, mg, osum, field_out, face_out, aux_out, rim, aux_held, sem, rim_sem
):
    _, planes, rows, width = field.shape
    cols = width // LANES
    outer = (0, rows // 8 - 1)
    places = [(comp, slice(1, planes - 1), pl.ds(8, rows - 16)) for comp in range(3)]
    places += [(slice(None), k) for k in (0, planes - 1)]
    stores = [
        pltpu.make_async_copy(field.at[place], field_out.at[place], sem.at[i])
        for i, place in enumerate(places)
    ]
    stores.append(pltpu.make_async_copy(face, face_out, sem.at[5]))
    for copy in stores:
        copy.start()

    def aux_store(side):
        return pltpu.make_async_copy(aux_held.at[side], aux_out.at[0, side], sem.at[6 + side])

    for side in range(2):

        @pl.loop(0, 2)
        def _(comp):
            for r in range(rows // 8):
                for c in range(cols):
                    place = (comp, pl.ds(8 * r, 8), pl.ds(c * LANES, LANES))
                    image = osum[(side, *place)]
                    for j in range(TERMS):
                        aux_held[(side, j, *place)] = image - aux[(0, side, j, *place)]

        aux_store(side).start()

    def rim_store(step, i):
        return pltpu.make_async_copy(
            rim.at[i, :, pl.ds(2 * step, 2)],
            field_out.at[:, pl.ds(1 + 2 * step, 2), pl.ds(8 * outer[i], 8)],
            rim_sem.at[i, step],
        )

    steps = planes // 2 - 1

    @pl.loop(0, steps)
    def _(step):
        for i, r in enumerate(outer):

            def write(place, news, g, c):
                for comp in range(3):
                    rim[i, comp, place[0] - 1, :, pl.ds(c * LANES, LANES)] = news[comp]

            sweep(e1, cur, mg, 1 + 2 * step, 2, r, False, write)
            rim_store(step, i).start()

    for copy in (*stores, aux_store(0), aux_store(1)):
        copy.wait()

    @pl.loop(0, steps)
    def _(step):
        for i in range(2):
            rim_store(step, i).wait()


def solution(mesh):
    n_slab, n_tile = mesh.shape["slab"], mesh.shape["tile"]

    def step(electric, current, mass_shift, interface, auxiliary):
        _, planes, rows, width = electric.shape
        cols = width // LANES
        tall = rows + 2 * PAD
        f32 = jnp.float32
        hbm = pl.BlockSpec(memory_space=pltpu.MemorySpace.HBM)
        vmem = pl.BlockSpec(memory_space=pltpu.VMEM)
        shapes = (electric.shape, interface.shape, auxiliary.shape)
        padded = (3, planes + 2, cols, tall, LANES)
        faces = (2, 2, rows, width)
        held_shapes = (*shapes, padded, electric.shape, mass_shift.shape, faces)
        held_bytes = sum(4 * math.prod(shape) for shape in held_shapes)

        def lines(n):
            return pltpu.VMEM((n, cols, LANES), f32)

        held = pl.pallas_call(
            functools.partial(kernel, n_slab, n_tile),
            out_shape=tuple(pltpu.VMEM(shape, f32) for shape in held_shapes),
            in_specs=[hbm] * 5,
            out_specs=(vmem,) * 7,
            scratch_shapes=[
                pltpu.VMEM(padded, f32),
                pltpu.VMEM((2, TERMS, 2, cols, tall, LANES), f32),
                pltpu.VMEM((6, cols, tall, LANES), f32),
                pltpu.VMEM((4, cols, tall, LANES), f32),
                pltpu.VMEM(faces, f32),
                *[lines(2 * planes)] * 4,
                *[lines(4 * TERMS)] * 4,
                *[lines(2 * planes + 10)] * 4,
                pltpu.SemaphoreType.DMA((10, cols)),
                pltpu.SemaphoreType.DMA((8, 2)),
                pltpu.SemaphoreType.DMA((8, 2)),
            ],
            compiler_params=pltpu.CompilerParams(
                collective_id=0,
                has_side_effects=True,
                vmem_limit_bytes=VMEM_TOTAL - held_bytes,
            ),
        )(electric, current, mass_shift, interface, auxiliary)
        return pl.pallas_call(
            store_kernel,
            out_shape=tuple(jax.ShapeDtypeStruct(shape, f32) for shape in shapes),
            in_specs=[vmem] * 7,
            out_specs=(hbm, hbm, hbm),
            scratch_shapes=[
                pltpu.VMEM((2, 3, planes - 2, 8, width), f32),
                pltpu.VMEM((2, TERMS, 2, rows, width), f32),
                pltpu.SemaphoreType.DMA((8,)),
                pltpu.SemaphoreType.DMA((2, planes // 2 - 1)),
            ],
            compiler_params=pltpu.CompilerParams(
                vmem_limit_bytes=8 * 2**20
            ),
        )(*held)

    placed = (
        P(None, "slab", "tile", None),
        P(None, "slab", "tile", None),
        P("slab", "tile", None),
        P("slab", None, None, "tile", None),
        P("slab", None, None, None, "tile", None),
    )
    return jax.shard_map(
        step,
        mesh=mesh,
        in_specs=placed,
        out_specs=(
            P(None, "slab", "tile", None),
            P("slab", None, None, "tile", None),
            P("slab", None, None, None, "tile", None),
        ),
        check_vma=False,
    )
```
